128 devices in a mesh: dp: 16 (over z, x), mp: 8 (over y, core).
Axes of the slice: x: 4, y: 4, z: 4, core: 2. Of those that a mesh axis runs over, the one named last changes fastest.
Arguments:
- hash_codes: int32 [16384, 2048], P('dp'), may hold values from 0 to 32703, as said below
- w_hash: bfloat16 [2048, 8192], P(None, 'mp'), may hold values from -0.125 to 0.125
- norm_gain: float32 [8192], P('mp'), may hold values from 0.1 to 1.9
- norm_bias: float32 [8192], P('mp'), may hold values from -3 to 3
- w_out: bfloat16 [8192, 256], P('mp'), may hold values from -0.0625 to 0.0625
- dense_vectors: bfloat16 [16384, 8, 256], P('dp'), may hold values from -6 to 6
- field_mix: float32 [8], replicated, may hold values from -3 to 3
- labels: int32 [16384], P('dp'), may hold values 0 or 1
Outputs:
- grad_hash: float32 [2048, 8192], P('dp', 'mp')
- grad_gain: float32 [8192], P('mp')
- grad_bias: float32 [8192], P('mp')
- grad_out: float32 [8192, 256], P('mp')
- mean_loss: float32 [], replicated
The draws below stay inside these ranges and needn't reach their ends.
Inputs may be any that keep to these rules, and one draw needn't show every extreme that they name: `hash_codes`: codes of fixed universal hashes of each id.
All inputs are finite; a program needn't handle non-finite values. No bound on the sum of `labels` on one device may be relied on, other than what follows from the above.
Results may differ from the reference program's by a relative error of at most 0.011.
Values may be sent and summed in bfloat16 or wider, within the bound.
No kernel may reach another device: no remote copies, remote signals or barrier semaphores. Data moves between devices by JAX's collectives and lax.ppermute only.
A program may use at most 192 MiB of HBM per device.

```python
import math
import jax
import jax.numpy as jnp
from jax import lax

CODES = 2048
UNITS = 8192
EMB = 256
FIELDS = 8
TOTAL = 16384


def draw_hash_codes(key, part):
    row_index = jnp.arange(TOTAL, dtype=jnp.int32)
    limits = 10902 + row_index * 21802 // (TOTAL - 1)
    codes = jax.random.randint(key, (TOTAL, CODES), 0, limits[:, None], dtype=jnp.int32)
    column_index = jnp.arange(CODES, dtype=jnp.int32)
    top_spot = (row_index[:, None] == TOTAL - 1) & (column_index[None, :] == 0)
    low_spot = (row_index[:, None] == 0) & (column_index[None, :] == 0)
    codes = jnp.where(top_spot, 32703, codes)
    codes = jnp.where(low_spot, 0, codes)
    return codes.astype(jnp.int32)


def place_ends(array, rng, least, high):
    longest = array.shape.index(max(array.shape))
    spots = []
    for shift in (0, 1):
        where = [jax.random.randint(jax.random.fold_in(rng, axis), (), 0, length) for axis, length in enumerate(array.shape)]
        where[longest] = (where[longest] + shift) % array.shape[longest]
        spots.append(tuple(where))
    return array.at[spots[0]].set(least).at[spots[1]].set(high)


def steps_of(own_key, dims, shards, least, top_value):
    def one(position, parts):
        heights = jax.random.uniform(jax.random.fold_in(jax.random.fold_in(own_key, 6), position), (parts,), jnp.float32, least / len(shards), top_value / len(shards))
        return jnp.repeat(jnp.exp(heights), dims[position] // parts).reshape((-1,) + (1,) * (len(dims) - position - 1))

    level = one(*shards[0])
    for cut in shards[1:]:
        level = level * one(*cut)
    return level


def bell_draw(own_key, dims, width, limit, cuts=(), held_as=jnp.bfloat16):
    values = jax.random.normal(own_key, dims, jnp.float32) * width
    if len(cuts) > 0:
        values = steps_of(own_key, dims, cuts, -0.22, 0.18) * values
    return jnp.clip(values, min=-limit, max=limit).astype(held_as)


def setup_inputs(seed: int = 0) -> dict:
    streams_of = jax.random.split(jax.random.key(seed), 9)
    hash_codes = draw_hash_codes(jax.random.fold_in(streams_of[8], 71), 0)
    w_hash = bell_draw(streams_of[1], (CODES, UNITS), CODES ** -0.5, 0.125, ((1, 8),))
    norm_gain = jnp.clip(1.0 + 0.18 * jax.random.normal(streams_of[2], (UNITS,), jnp.float32), 0.1, 1.9)
    norm_bias = bell_draw(streams_of[3], (UNITS,), 0.5, 3.0, ((0, 8),), jnp.float32)
    w_out = bell_draw(streams_of[4], (UNITS, EMB), UNITS ** -0.5, 0.0625, ((0, 8),))
    dense_vectors = bell_draw(streams_of[5], (TOTAL, FIELDS, EMB), 1.0, 6.0, ((0, 16),))
    field_mix = bell_draw(streams_of[6], (FIELDS,), 1.0, 3.0, (), jnp.float32)
    labels = place_ends((jax.random.randint(streams_of[7], (TOTAL,), 0, 2) < 1).astype(jnp.int32), jax.random.fold_in(streams_of[7], 1), 0, 1)
    return dict(hash_codes=hash_codes, w_hash=w_hash, norm_gain=norm_gain, norm_bias=norm_bias, w_out=w_out, dense_vectors=dense_vectors, field_mix=field_mix, labels=labels)


buckets = 32704.0
epsilon = 1e-05
grad_scale = 32.0

def mish_parts(pre_act):
    softer = jax.nn.softplus(pre_act)
    tangent = jnp.tanh(softer)
    value = pre_act * tangent
    mish_slope = tangent + pre_act * jax.nn.sigmoid(pre_act) * (1.0 - tangent * tangent)
    return (value, mish_slope)

def reference(hash_codes, w_hash, norm_gain, norm_bias, w_out, dense_vectors, field_mix, labels):
    total_rows = hash_codes.shape[0]
    inputs = (hash_codes.astype(jnp.float32) * (2.0 / (buckets - 1.0)) - 1.0).astype(jnp.bfloat16)
    pre_act = jnp.dot(inputs, w_hash, preferred_element_type=jnp.float32)
    hidden, mish_slope = mish_parts(pre_act)
    unit_mean = lax.optimization_barrier(jnp.sum(hidden, 0)) / total_rows
    unit_var = lax.optimization_barrier(jnp.sum(hidden * hidden, 0)) / total_rows - unit_mean * unit_mean
    inv_std = lax.rsqrt(unit_var + epsilon)
    centred = (hidden - unit_mean) * inv_std
    normed = (norm_gain * centred + norm_bias).astype(jnp.bfloat16)
    embedding = jnp.dot(normed, w_out, preferred_element_type=jnp.float32)
    dense_wide = dense_vectors.astype(jnp.float32)
    scores = lax.optimization_barrier(jnp.sum(embedding[:, None, :] * dense_wide, -1))
    logits = lax.optimization_barrier(jnp.sum(scores * field_mix, -1)) / math.sqrt(EMB)
    targets = labels.astype(jnp.float32)
    mean_loss = jnp.sum(jax.nn.softplus(logits) - targets * logits) / total_rows
    grad_logits = (jax.nn.sigmoid(logits) - targets) * (grad_scale / math.sqrt(total_rows))
    grad_scores = grad_logits[:, None] * field_mix / math.sqrt(EMB)
    grad_embed = lax.optimization_barrier(jnp.sum(grad_scores[:, :, None] * dense_wide, 1)).astype(jnp.bfloat16)
    grad_out = lax.dot_general(normed, grad_embed, (((0,), (0,)), ((), ())), preferred_element_type=jnp.float32)
    grad_normed = lax.dot_general(grad_embed, w_out, (((1,), (1,)), ((), ())), preferred_element_type=jnp.float32)
    grad_bias = lax.optimization_barrier(jnp.sum(grad_normed, 0))
    grad_gain = lax.optimization_barrier(jnp.sum(grad_normed * centred, 0))
    grad_hidden = inv_std * (norm_gain * grad_normed - norm_gain * grad_bias / total_rows - centred * norm_gain * grad_gain / total_rows)
    grad_pre = (grad_hidden * mish_slope).astype(jnp.bfloat16)
    grad_hash = lax.dot_general(inputs, grad_pre, (((0,), (0,)), ((), ())), preferred_element_type=jnp.float32)
    return (grad_hash, grad_gain, grad_bias, grad_out, mean_loss)
```

```python
import math

import jax
import jax.numpy as jnp
from jax import lax
from jax.sharding import Mesh
from jax.sharding import PartitionSpec as P

EMB = 256
DP = ("z", "x")
buckets = 32704.0
epsilon = 1e-05
grad_scale = 32.0
EXP_TOP = 20.0


def hop(value, axis, step):
    count = lax.axis_size(axis)
    return lax.ppermute(value, axis, [(i, (i + step) % count) for i in range(count)])


def ring_total(value, axis):
    count = lax.axis_size(axis)
    total = value
    for part in [hop(value, axis, step) for step in range(1, count)]:
        total = total + part
    return total


def dp_total(value):
    return ring_total(ring_total(value, "z"), "x")


def mp_total(value):
    return ring_total(ring_total(value, "core"), "y")


def wide_add(a, b):
    return (a.astype(jnp.float32) + b.astype(jnp.float32)).astype(jnp.bfloat16)


def sum_scatter(piece, axis):
    me = lax.axis_index(axis)
    up, down, far = (me + 1) % 4, (me + 3) % 4, (me + 2) % 4
    right = hop(jnp.stack([piece(far, 0), piece(up, 1)]), axis, 1)
    left = hop(jnp.stack([piece(far, 1), piece(down, 0)]), axis, -1)
    right_two = hop(wide_add(right[0], piece(up, 0)), axis, 1)
    left_two = hop(wide_add(left[0], piece(down, 1)), axis, -1)
    own = piece(me, 0).astype(jnp.float32) + left[1].astype(jnp.float32) + right_two.astype(jnp.float32)
    own_two = piece(me, 1).astype(jnp.float32) + right[1].astype(jnp.float32) + left_two.astype(jnp.float32)
    return own, own_two


def grid_scatter(part, cols):
    quarter = cols // 4

    def first(axis_dim, base):
        def piece(chunk, half):
            held = lax.dynamic_index_in_dim(part, chunk, axis_dim, keepdims=False)
            return held[..., base + half * quarter : base + (half + 1) * quarter]

        return piece

    def second(halves):
        joined = jnp.stack([h.astype(jnp.bfloat16) for h in halves], 0)

        def piece(chunk, half):
            return lax.dynamic_index_in_dim(joined[half], chunk, 0, keepdims=False)

        return piece

    z_first = sum_scatter(first(0, 0), "z")
    x_first = sum_scatter(first(1, 2 * quarter), "x")
    a = sum_scatter(second(z_first), "x")
    b = sum_scatter(second(x_first), "z")
    return jnp.concatenate([*a, *b], -1)


def on_device(hash_codes, w_hash, norm_gain, norm_bias, w_out, dense_vectors, field_mix, labels):
    rows = hash_codes.shape[0]
    units = w_hash.shape[1]
    total_rows = rows * lax.axis_size(DP)
    inputs = (hash_codes.astype(jnp.float32) * (2.0 / (buckets - 1.0)) - 1.0).astype(jnp.bfloat16)
    pre_act = jnp.dot(inputs, w_hash, preferred_element_type=jnp.float32)
    grown = jnp.exp(jnp.minimum(pre_act, EXP_TOP))
    both = grown * (grown + 2.0)
    inverse = 1.0 / (both + 2.0)
    tangent = both * inverse
    hidden = pre_act * tangent
    slope = tangent + pre_act * (4.0 * grown * (1.0 + grown)) * (inverse * inverse)
    sums = dp_total(jnp.stack([jnp.sum(hidden, 0), jnp.sum(hidden * hidden, 0)]))
    mixed = jnp.einsum("rfe,f->re", dense_vectors.astype(jnp.float32), field_mix / math.sqrt(EMB), precision="highest")
    spread = lax.dot_general(
        mixed.astype(jnp.bfloat16), w_out, (((1,), (1,)), ((), ())), preferred_element_type=jnp.float32
    )
    unit_mean = sums[0] / total_rows
    unit_var = sums[1] / total_rows - unit_mean * unit_mean
    inv_std = lax.rsqrt(unit_var + epsilon)
    centred = (hidden - unit_mean) * inv_std
    normed = norm_gain * centred + norm_bias
    logits = mp_total(jnp.sum(normed * spread, 1))
    targets = labels.astype(jnp.float32)
    loss_local = jnp.sum(jax.nn.softplus(logits) - targets * logits)
    grad_logits = (jax.nn.sigmoid(logits) - targets) * (grad_scale / math.sqrt(total_rows))
    grad_normed = grad_logits[:, None] * spread
    grad_sums = dp_total(
        jnp.stack([jnp.sum(grad_normed, 0), jnp.sum(grad_normed * centred, 0), jnp.full((units,), loss_local)])
    )
    grad_bias, grad_gain = grad_sums[0], grad_sums[1]
    mean_loss = grad_sums[2, 0] / total_rows
    grad_embed = (grad_logits[:, None] * mixed).astype(jnp.bfloat16)
    out_local = lax.dot_general(
        normed.astype(jnp.bfloat16), grad_embed, (((0,), (0,)), ((), ())), preferred_element_type=jnp.float32
    ).astype(jnp.bfloat16)
    out_own = grid_scatter(out_local.reshape(4, 4, units // 16, EMB), EMB).astype(jnp.bfloat16)
    out_all = lax.all_gather(lax.all_gather(out_own, "x"), "z")
    grad_out = out_all.reshape(units, EMB).astype(jnp.float32)
    grad_hidden = inv_std * (
        norm_gain * grad_normed
        - norm_gain * grad_bias / total_rows
        - centred * norm_gain * grad_gain / total_rows
    )
    grad_pre = (grad_hidden * slope).astype(jnp.bfloat16)
    hash_local = lax.dot_general(
        inputs, grad_pre, (((0,), (0,)), ((), ())), preferred_element_type=jnp.float32
    ).astype(jnp.bfloat16)
    grad_hash = grid_scatter(hash_local.reshape(4, 4, hash_local.shape[0] // 16, units), units)
    return (grad_hash, grad_gain, grad_bias, grad_out, mean_loss)


def solution(mesh):
    split = Mesh(mesh.devices.reshape(4, 4, 4, 2), ("z", "x", "y", "core"))
    mp = ("y", "core")
    return jax.shard_map(
        on_device,
        mesh=split,
        in_specs=(P(DP, None), P(None, mp), P(mp), P(mp), P(mp, None), P(DP, None, None), P(), P(DP)),
        out_specs=(P(DP, mp), P(mp), P(mp), P(mp, None), P()),
        check_vma=False,
    )
```

```python
import functools
import math

import jax
import jax.numpy as jnp
from jax import lax
from jax.experimental import pallas as pl
from jax.experimental.pallas import tpu as pltpu
from jax.sharding import Mesh
from jax.sharding import PartitionSpec as P

DP = ("z", "x")
MP = ("y", "core")
buckets = 32704.0
epsilon = 1e-05
grad_scale = 32.0
EXP_TOP = 20.0
LANES = 128
F32 = jnp.float32
BF16 = jnp.bfloat16
MIB = 1024 * 1024


def hop(value, axis, step):
    count = lax.axis_size(axis)
    return lax.ppermute(value, axis, [(i, (i + step) % count) for i in range(count)])


def exchange(blocks, axes):
    return lax.all_to_all(blocks, axes, 0, 0, tiled=True)


def call(body, ins, outs, scratch=(), flops=0, limit=16, name=None):
    place = {"v": pltpu.VMEM, "h": pltpu.HBM, "a": pl.ANY, "s": pltpu.SMEM, "p": pltpu.VMEM}
    held = {"p": pltpu.VMEM, "h": pltpu.HBM}
    arrays = [pltpu.with_memory_space_constraint(a, held[s]) if s in held else a for a, s in ins]
    shapes = [
        held[s](shape, dtype) if s in held else jax.ShapeDtypeStruct(shape, dtype) for shape, dtype, s in outs
    ]
    return pl.pallas_call(
        body,
        out_shape=shapes,
        in_specs=[pl.BlockSpec(memory_space=place[s]) for _, s in ins],
        out_specs=[pl.BlockSpec(memory_space=place[s]) for _, _, s in outs],
        scratch_shapes=list(scratch),
        cost_estimate=pl.CostEstimate(flops=flops, bytes_accessed=0, transcendentals=0),
        compiler_params=pltpu.CompilerParams(vmem_limit_bytes=limit * MIB),
        name=name,
    )(*arrays)


def dot(a, b):
    return jnp.dot(a, b, preferred_element_type=F32)


def span(i, size):
    return pl.ds(pl.multiple_of(i * size, size), size)


def rows_in(hbm, held, sems, k, i, size):
    at = span(i, size)
    return pltpu.make_async_copy(hbm.at[at, :], held.at[at, :], sems.at[k, i])


def as_inputs(codes):
    return (codes.astype(F32) * (2.0 / (buckets - 1.0)) - 1.0).astype(BF16)


def decode_body(codes_hbm, w_hbm, hidden_hbm, slope_hbm, sums, codes, weights, hidden, slope, inputs, pre_a, pre_b, totals,
                code_sem, w_sem, out_sem):
    rows, units = hidden.shape
    block, tile = pre_a.shape
    blocks, tiles = rows // block, units // tile
    pres = (pre_a, pre_b)
    part, strip = 32, 256

    def fetch(i):
        at = slice(i * block, (i + 1) * block)
        return pltpu.make_async_copy(codes_hbm.at[at, :], codes.at[at, :], code_sem.at[i])

    def fetch_w(n):
        cols = pl.ds(n * tile, tile)
        return pltpu.make_async_copy(w_hbm.at[:, cols], weights.at[:, cols], w_sem.at[n])

    def put(k, i):
        held, hbm = ((hidden, hidden_hbm), (slope, slope_hbm))[k]
        at = slice(i * block, (i + 1) * block)
        return pltpu.make_async_copy(held.at[at, :], hbm.at[at, :], out_sem.at[k, i])

    fetch(0).start()
    fetch_w(0).start()
    fetch_w(1).start()
    for i in range(1, blocks):
        fetch(i).start()
    totals[...] = jnp.zeros_like(totals)

    def convert(i):
        fetch(i).wait()
        for r in range(block // part):
            at = slice(i * block + r * part, i * block + (r + 1) * part)
            inputs[at, :] = as_inputs(codes[at, :])

    def finish(i, n):
        for c in range(tile // strip):
            cols = slice(n * tile + c * strip, n * tile + (c + 1) * strip)
            first = jnp.zeros((8, strip), F32)
            second = jnp.zeros((8, strip), F32)
            for r in range(block // part):
                at = slice(i * block + r * part, i * block + (r + 1) * part)
                x = pres[n][r * part : (r + 1) * part, c * strip : (c + 1) * strip]
                grown = jnp.exp(jnp.minimum(x, EXP_TOP))
                both = grown * (grown + 2.0)
                inverse = 1.0 / (both + 2.0)
                tangent = both * inverse
                value = x * tangent
                hidden[at, cols] = value
                slope[at, cols] = (tangent + (x * (4.0 * inverse)) * ((grown + grown * grown) * inverse)).astype(BF16)
                first = first + value.reshape(part // 8, 8, strip).sum(0)
                second = second + (value * value).reshape(part // 8, 8, strip).sum(0)
            totals[0:8, cols] += first
            totals[8:16, cols] += second

    convert(0)
    last = None
    for i in range(blocks):
        at = slice(i * block, (i + 1) * block)
        for n in range(tiles):
            if i == 0:
                fetch_w(n).wait()
            if n == tiles - 1 and i + 1 < blocks:
                convert(i + 1)
            pres[n][...] = dot(inputs[at, :], weights[:, n * tile : (n + 1) * tile])
            if last is not None:
                finish(*last)
                if last[1] == tiles - 1:
                    put(0, last[0]).start()
                    put(1, last[0]).start()
            last = (i, n)
    finish(*last)
    put(0, blocks - 1).start()
    put(1, blocks - 1).start()
    first = jnp.sum(totals[0:8, :], 0, keepdims=True)
    second = jnp.sum(totals[8:16, :], 0, keepdims=True)
    for k in range(sums.shape[0]):
        sums[k, 0:1, :] = first
        sums[k, 1:2, :] = second
    for i in range(blocks):
        for k in range(2):
            put(k, i).wait()


def turn_body(codes_hbm, after, turned_hbm, codes, turned, sem, out_sem):
    del after
    rows = codes.shape[0]
    block = LANES
    blocks = rows // block

    def put(i):
        at = span(i, block)
        return pltpu.make_async_copy(turned.at[:, at], turned_hbm.at[:, at], out_sem.at[i])

    for i in range(blocks):
        rows_in(codes_hbm, codes, sem, 0, i, block).start()

    def step(i, carry):
        at = span(i, block)
        rows_in(codes_hbm, codes, sem, 0, i, block).wait()
        for q in range(codes.shape[1] // 256):
            cols = slice(q * 256, (q + 1) * 256)
            turned[cols, at] = as_inputs(codes[at, cols]).T
        put(i).start()
        return carry

    lax.fori_loop(0, blocks, step, 0)
    for i in range(blocks):
        put(i).wait()


def mix_body(after, dense_hbm, mix, w_out, spread_hbm, mixed_t, dense, mixed, spread, sem, out_sem):
    del after
    rows = spread.shape[0]
    block = 64
    deep = dense.shape[1]
    fields = deep // block
    pairs = rows // (2 * block)
    group = rows // 2

    def fetch(i):
        return pltpu.make_async_copy(dense_hbm.at[span(i, deep), :], dense.at[i], sem.at[i])

    def put(i):
        at = slice(i * group, (i + 1) * group)
        return pltpu.make_async_copy(spread.at[at, :], spread_hbm.at[at, :], out_sem.at[i])

    for i in range(2 * pairs):
        fetch(i).start()
    high = mix[...].astype(BF16)
    low = (mix[...] - high.astype(F32)).astype(BF16)
    owner = lax.broadcasted_iota(jnp.int32, (block, deep), 1) // fields
    mine = owner == lax.broadcasted_iota(jnp.int32, (block, deep), 0)
    picks = jnp.concatenate(
        [jnp.where(mine, high.astype(F32), 0.0), jnp.where(mine, low.astype(F32), 0.0)], 0
    ).astype(BF16)

    def step(i, carry):
        fetch(2 * i).wait()
        fetch(2 * i + 1).wait()
        even = dot(picks, dense[2 * i])
        odd = dot(picks, dense[2 * i + 1])
        both = jnp.concatenate([even[:block] + even[block:], odd[:block] + odd[block:]], 0)
        at = span(i, 2 * block)
        mixed_t[:, at] = both.T
        mixed[at, :] = both.astype(BF16)
        return carry

    for g in range(2):
        lax.fori_loop(g * pairs // 2, (g + 1) * pairs // 2, step, 0)
        at = slice(g * group, (g + 1) * group)
        spread[at, :] = lax.dot_general(
            mixed[at, :], w_out[...], (((1,), (1,)), ((), ())), preferred_element_type=F32
        ).astype(BF16)
        put(g).start()
    for g in range(2):
        put(g).wait()


def logit_body(total_rows, arrived, gain, bias, hidden_hbm, spread_hbm, coef, parts, hidden, spread, sem):
    rows, units = hidden.shape
    block = LANES
    blocks = rows // block

    for i in range(blocks):
        rows_in(hidden_hbm, hidden, sem, 0, i, block).start()
        rows_in(spread_hbm, spread, sem, 1, i, block).start()
    stats = jnp.sum(arrived[...], 0)
    mean = stats[0:1] / total_rows
    var = stats[1:2] / total_rows - mean * mean
    inv = lax.rsqrt(var + epsilon)
    coef[0:1, :] = gain[...] * inv
    coef[1:2, :] = bias[...]
    coef[2:3, :] = mean
    coef[3:4, :] = inv

    def step(i, carry):
        at = span(i, block)
        rows_in(hidden_hbm, hidden, sem, 0, i, block).wait()
        rows_in(spread_hbm, spread, sem, 1, i, block).wait()
        total = jnp.zeros((block, LANES), F32)
        for n in range(units // LANES):
            cols = slice(n * LANES, (n + 1) * LANES)
            value = (hidden[at, cols] - coef[2:3, cols]) * coef[0:1, cols] + coef[1:2, cols]
            total = total + value * spread[at, cols].astype(F32)
        line = jnp.sum(total.T, 0, keepdims=True)
        for k in range(parts.shape[0]):
            parts[k, pl.ds(i, 1), :] = line
        return carry

    lax.fori_loop(0, blocks, step, 0)


def column(line):
    return jnp.broadcast_to(line, (LANES, LANES)).T


def three_parts(value):
    high = value.astype(BF16)
    rest = value - high.astype(F32)
    middle = rest.astype(BF16)
    return high, middle, (rest - middle.astype(F32)).astype(BF16)


def grad_body(total_rows, arrived, labels, hidden_hbm, spread_hbm, coef, mixed_t, grads, packed, hidden, spread,
              normed, weighted, totals, sem):
    rows, units = hidden.shape
    emb = mixed_t.shape[0]
    block = LANES
    blocks = rows // block
    own = packed.shape[0]
    share = units // own
    for i in range(blocks):
        rows_in(hidden_hbm, hidden, sem, 0, i, block).start()
        rows_in(spread_hbm, spread, sem, 1, i, block).start()
    logits = jnp.sum(arrived[...], 0)
    targets = labels[...]
    positive = jnp.maximum(logits, 0.0) + jnp.log1p(jnp.exp(-jnp.abs(logits)))
    loss = jnp.sum(positive - targets * logits, keepdims=True)
    grads[...] = (jax.nn.sigmoid(logits) - targets) * (grad_scale / math.sqrt(total_rows))
    for i in range(blocks):
        at = slice(i * block, (i + 1) * block)
        weighted[:, at] = (mixed_t[:, at] * grads[i : i + 1, :]).astype(BF16)
    totals[...] = jnp.zeros_like(totals)

    def step(i, carry):
        at = span(i, block)
        rows_in(hidden_hbm, hidden, sem, 0, i, block).wait()
        rows_in(spread_hbm, spread, sem, 1, i, block).wait()
        weight = column(grads[pl.ds(i, 1), :])
        for n in range(units // LANES):
            cols = slice(n * LANES, (n + 1) * LANES)
            part = weight * spread[at, cols].astype(F32)
            centred = hidden[at, cols] - coef[2:3, cols]
            normed[at, cols] = (centred * coef[0:1, cols] + coef[1:2, cols]).astype(BF16)
            product = part * centred
            totals[0:8, cols] += part.reshape(block // 8, 8, LANES).sum(0)
            totals[8:16, cols] += product.reshape(block // 8, 8, LANES).sum(0)
        return carry

    lax.fori_loop(0, blocks, step, 0)
    bias = jnp.sum(totals[0:8, :], 0, keepdims=True)
    gain = jnp.sum(totals[8:16, :], 0, keepdims=True) * coef[3:4, :]
    cuts = [slice(q * emb, (q + 1) * emb) for q in range(units // emb)]
    lines = jnp.concatenate([bias[:, c] for c in cuts] + [gain[:, c] for c in cuts], 0)
    spare = [v.astype(F32) for v in three_parts(jnp.broadcast_to(loss, (1, emb)))]
    extra = jnp.concatenate(spare + [jnp.zeros((5, emb), F32)], 0).astype(BF16)
    for p, block_of in enumerate((*three_parts(lines), extra)):
        for k in range(own):
            packed[k, share + 8 * p : share + 8 * p + 8, :] = block_of
    for n in range(units // 512):
        cols = slice(n * 512, (n + 1) * 512)
        out = dot(weighted[...], normed[:, cols]).T.astype(BF16)
        for k in range(512 // share):
            packed[n * (512 // share) + k, 0:share, :] = out[k * share : (k + 1) * share, :]


def back_body(total_rows, arrived, grads, hidden_hbm, spread_hbm, slope_hbm, coef, grad_pre, grad_gain, grad_bias, loss,
              piece, hidden, spread, slope, both, sem):
    rows, units = hidden.shape
    block = LANES
    blocks = rows // block
    share, emb = piece.shape
    for i in range(blocks):
        rows_in(hidden_hbm, hidden, sem, 0, i, block).start()
        rows_in(spread_hbm, spread, sem, 1, i, block).start()
        rows_in(slope_hbm, slope, sem, 2, i, block).start()
    count = units // emb

    def stat(p):
        return jnp.sum(arrived[:, share + 8 * p : share + 8 * p + 8, :].astype(F32), 0)

    lines = (stat(2) + stat(1)) + stat(0)
    for q in range(count):
        cols = slice(q * emb, (q + 1) * emb)
        grad_bias[:, cols] = lines[q : q + 1]
        grad_gain[:, cols] = lines[count + q : count + q + 1]
        both[0:1, cols] = lines[q : q + 1] / total_rows
        both[1:2, cols] = lines[count + q : count + q + 1] * coef[3:4, cols] / total_rows
    loss[...] = jnp.sum(stat(3), 0, keepdims=True)[:, 0:LANES] / total_rows
    piece[...] = jnp.sum(arrived[:, 0:share, :].astype(F32), 0).astype(BF16)

    def step(i, carry):
        at = span(i, block)
        rows_in(hidden_hbm, hidden, sem, 0, i, block).wait()
        rows_in(spread_hbm, spread, sem, 1, i, block).wait()
        rows_in(slope_hbm, slope, sem, 2, i, block).wait()
        weight = column(grads[pl.ds(i, 1), :])
        for n in range(units // LANES):
            cols = slice(n * LANES, (n + 1) * LANES)
            inner = weight * spread[at, cols].astype(F32) - both[0:1, cols]
            inner = inner - (hidden[at, cols] - coef[2:3, cols]) * both[1:2, cols]
            grad_pre[at, cols] = (inner * coef[0:1, cols] * slope[at, cols].astype(F32)).astype(BF16)
        return carry

    lax.fori_loop(0, blocks, step, 0)


def product_body(jobs, keep, chunks, turned, grad_pre, piece, after, *refs):
    del after
    count = len(jobs)
    outs, (lines, held, sem) = refs[:count], refs[count:]
    rows = lines.shape[0]
    wide = held.shape[2]
    some = held.shape[1] - rows
    sub = rows // 4

    def put(k):
        return pltpu.make_async_copy(held.at[k], outs[k], sem.at[k])

    for k, (axis, place) in enumerate(jobs):
        c = chunks[place]
        out = outs[k] if keep else held.at[k]
        if axis == "z":
            left = turned[span(c, rows), :]
            base, first = 0, 0
        else:
            for q in range(4):
                at = pl.ds(pl.multiple_of(q * rows + c * sub, sub), sub)
                lines[q * sub : (q + 1) * sub, :] = turned[at, :]
            left = lines[...]
            base, first = wide, 2 * some
        out[0:rows, :] = dot(left, grad_pre[:, base : base + wide]).astype(BF16)
        for n in range(2):
            out[rows:, n * 256 : (n + 1) * 256] = piece[first + n * some : first + (n + 1) * some, :]
        if not keep:
            put(k).start()
    if not keep:
        for k in range(count):
            put(k).wait()


def middle_body(chunk, own, far, up, down, own_out, far_out, up_out, down_out):
    me, was = chunk[0], chunk[1]
    rows = own_out.shape[0]
    full = own.shape[0] - (far_out.shape[0] - rows) // 4
    some = (far_out.shape[0] - rows) // 4
    for step, out in ((2, far_out), (1, up_out), (3, down_out), (0, own_out)):
        at = span(lax.rem(me + step, 4), rows)
        total = (own[at, :].astype(F32) + far[at, :].astype(F32)) + (up[at, :].astype(F32) + down[at, :].astype(F32))
        out[0:rows, :] = total.astype(out.dtype)
        if step:
            for back, came in ((0, own), (2, far), (1, up), (3, down)):
                to = pl.ds(pl.multiple_of(rows + lax.rem(was + 4 - back, 4) * some, some), some)
                out[to, :] = came[full:, :]


def last_body(place, own_a, a0, a2, a1, a3, own_b, b0, b2, b1, b3, grad_hash, grad_out):
    rows, half = own_a.shape
    some = (a0.shape[0] - rows) // 4
    share = 4 * some
    for base, own, came in ((0, own_a, (a2, a1, a3)), (half, own_b, (b2, b1, b3))):
        total = own[...]
        for part in came:
            total = total + part[0:rows, :].astype(F32)
        grad_hash[:, base : base + half] = total
    for kind, pieces in ((0, (a0, a2, a1, a3)), (1, (b0, b2, b1, b3))):
        me = place[1 - kind]
        for back, came in zip((0, 2, 1, 3), pieces):
            there = lax.rem(me + 4 - back, 4)
            for k in range(4):
                owner = k * 4 + there if kind == 0 else there * 4 + k
                for n in range(2):
                    to = pl.ds(pl.multiple_of(owner * share + (2 * kind + n) * some, some), some)
                    at = slice(rows + k * some, rows + (k + 1) * some)
                    grad_out[to, :] = came[at, n * 256 : (n + 1) * 256].astype(F32)


def on_device(hash_codes, w_hash, norm_gain, norm_bias, w_out, dense_vectors, field_mix, labels):
    rows, codes = hash_codes.shape
    units = w_hash.shape[1]
    fields, emb = dense_vectors.shape[1:]
    dp, mp = lax.axis_size(DP), lax.axis_size(MP)
    total_rows = rows * dp
    lines = rows // LANES
    half = units // 2
    share = units // dp
    some = share // 4
    dma = pltpu.SemaphoreType.DMA
    hidden, slope, sums = call(
        decode_body,
        [(hash_codes, "h"), (w_hash, "h")],
        [((rows, units), F32, "h"), ((rows, units), BF16, "h"), ((dp, 2, units), F32, "v")],
        [
            pltpu.VMEM((rows, codes), jnp.int32),
            pltpu.VMEM((codes, units), BF16),
            pltpu.VMEM((rows, units), F32),
            pltpu.VMEM((rows, units), BF16),
            pltpu.VMEM((rows, codes), BF16),
            pltpu.VMEM((256, units // 2), F32),
            pltpu.VMEM((256, units // 2), F32),
            pltpu.VMEM((16, units), F32),
            dma((rows // 256,)),
            dma((2,)),
            dma((2, rows // 256)),
        ],
        flops=2 * rows * codes * units,
        limit=40,
        name="decode",
    )
    arrived = exchange(sums, DP)
    mix_line = jnp.tile(field_mix / math.sqrt(emb), 64).reshape(1, fields * 64)
    spread, mixed_t = call(
        mix_body,
        [(sums, "a"), (dense_vectors.reshape(rows * fields, emb), "h"), (mix_line, "v"), (w_out, "v")],
        [((rows, units), BF16, "h"), ((emb, rows), F32, "v")],
        [
            pltpu.VMEM((rows // 64, fields * 64, emb), BF16),
            pltpu.VMEM((rows, emb), BF16),
            pltpu.VMEM((rows, units), BF16),
            dma((rows // 64,)),
            dma((2,)),
        ],
        flops=8 * rows * units * emb,
        limit=16,
        name="mix",
    )
    coef, parts = call(
        functools.partial(logit_body, float(total_rows)),
        [
            (arrived, "v"),
            (norm_gain.reshape(1, units), "v"),
            (norm_bias.reshape(1, units), "v"),
            (hidden, "h"),
            (spread, "h"),
        ],
        [((8, units), F32, "v"), ((mp, lines, LANES), F32, "v")],
        [pltpu.VMEM((rows, units), F32), pltpu.VMEM((rows, units), BF16), dma((2, lines))],
        limit=20,
        flops=4 * rows * units,
        name="logit",
    )
    logits = exchange(parts, MP)
    targets = labels.astype(F32).reshape(lines, LANES)
    grads, packed = call(
        functools.partial(grad_body, float(total_rows)),
        [(logits, "v"), (targets, "v"), (hidden, "h"), (spread, "h"), (coef, "v"), (mixed_t, "v")],
        [((lines, LANES), F32, "v"), ((dp, share + 32, emb), BF16, "v")],
        [
            pltpu.VMEM((rows, units), F32),
            pltpu.VMEM((rows, units), BF16),
            pltpu.VMEM((rows, units), BF16),
            pltpu.VMEM((emb, rows), BF16),
            pltpu.VMEM((16, units), F32),
            dma((2, lines)),
        ],
        limit=24,
        flops=2 * rows * units * emb,
        name="grad",
    )
    grad_arrived = exchange(packed, DP)
    (turned,) = call(
        turn_body,
        [(hash_codes, "h"), (grads, "a")],
        [((codes, rows), BF16, "h")],
        [pltpu.VMEM((rows, codes), jnp.int32), pltpu.VMEM((codes, rows), BF16), dma((1, lines)), dma((lines,))],
        flops=16 * rows * codes * LANES,
        limit=16,
        name="turn",
    )
    grad_pre, grad_gain, grad_bias, loss, piece = call(
        functools.partial(back_body, float(total_rows)),
        [(grad_arrived, "v"), (grads, "v"), (hidden, "h"), (spread, "h"), (slope, "h"), (coef, "v")],
        [
            ((rows, units), BF16, "p"),
            ((1, units), F32, "v"),
            ((1, units), F32, "v"),
            ((1, LANES), F32, "v"),
            ((share, emb), BF16, "p"),
        ],
        [
            pltpu.VMEM((rows, units), F32),
            pltpu.VMEM((rows, units), BF16),
            pltpu.VMEM((rows, units), BF16),
            pltpu.VMEM((8, units), F32),
            dma((3, lines)),
        ],
        limit=20,
        flops=8 * rows * units,
        name="back",
    )
    here = {axis: lax.axis_index(axis).astype(jnp.int32) for axis in DP}

    chunks = jnp.stack([(here[axis] + step) & 3 for axis in DP for step in range(4)])

    def products(steps, keep, after, name):
        jobs = [(axis, 4 * DP.index(axis) + step) for step in steps for axis in DP]
        size = (codes // 4 + some, half)
        outs = call(
            functools.partial(product_body, jobs, keep),
            [(chunks, "s"), (turned, "p"), (grad_pre, "p"), (piece, "p"), (after, "a")],
            [(size, BF16, "p" if keep else "h")] * len(jobs),
            [pltpu.VMEM((codes // 4, rows), BF16), pltpu.VMEM((1 if keep else len(jobs), *size), BF16), dma((len(jobs),))],
            flops=2 * rows * half * (codes // 4) * len(jobs),
            limit=8,
            name=name,
        )
        return {(axis, place & 3): out for (axis, place), out in zip(jobs, outs)}

    made = products((2,), False, grads, "product_far")
    made.update(products((1, 3), False, made["z", 2], "product_near"))
    made.update(products((0,), True, made["z", 1], "product_own"))
    got = {(axis, step): hop(made[axis, step], axis, step) for step in (2, 1, 3) for axis in DP}
    other = {"z": "x", "x": "z"}
    last = []
    for axis in DP:
        own, far, up, down = call(
            middle_body,
            [(jnp.stack([here[other[axis]], here[axis]]), "s"), (made[axis, 0], "p")]
            + [(got[axis, step], "p") for step in (2, 1, 3)],
            [((codes // 16, half), F32, "p")] + [((codes // 16 + 4 * some, half), BF16, "p")] * 3,
            limit=4,
            flops=rows * units,
            name="middle_" + axis,
        )
        last += [own, far] + [hop(v, other[axis], step) for v, step in ((far, 2), (up, 1), (down, 3))]
    grad_hash, grad_out = call(
        last_body,
        [(jnp.stack([here["z"], here["x"]]), "s")] + [(v, "p") for v in last],
        [((codes // 16, units), F32, "v"), ((units, emb), F32, "v")],
        limit=8,
        flops=rows * units,
        name="last",
    )
    return (grad_hash, grad_gain.reshape(units), grad_bias.reshape(units), grad_out, loss[0, 0])


def solution(mesh):
    split = Mesh(mesh.devices.reshape(4, 4, 4, 2), ("z", "x", "y", "core"))
    return jax.shard_map(
        on_device,
        mesh=split,
        in_specs=(P(DP, None), P(None, MP), P(MP), P(MP), P(MP, None), P(DP, None, None), P(), P(DP)),
        out_specs=(P(DP, MP), P(MP), P(MP), P(MP, None), P()),
        check_vma=False,
    )
```

```python
import functools
import math

import jax
import jax.numpy as jnp
from jax import lax
from jax.experimental import pallas as pl
from jax.experimental.pallas import tpu as pltpu
from jax.sharding import Mesh
from jax.sharding import PartitionSpec as P


DP = ("z", "x")
MP = ("y", "core")
buckets = 32704.0
epsilon = 1e-05
grad_scale = 32.0
EXP_TOP = 20.0
LANES = 128
F32 = jnp.float32
BF16 = jnp.bfloat16
MIB = 1024 * 1024


def hop(value, axis, step):
    count = lax.axis_size(axis)
    return lax.ppermute(value, axis, [(i, (i + step) % count) for i in range(count)])


def exchange(blocks, axes):
    return lax.all_to_all(blocks, axes, 0, 0, tiled=True)


def call(body, ins, outs, scratch=(), flops=0, limit=16):
    place = {"v": pltpu.VMEM, "h": pltpu.HBM, "a": pl.ANY, "s": pltpu.SMEM, "p": pltpu.VMEM}
    held = {"p": pltpu.VMEM, "h": pltpu.HBM}
    arrays = [pltpu.with_memory_space_constraint(a, held[s]) if s in held else a for a, s in ins]
    shapes = [
        held[s](shape, dtype) if s in held else jax.ShapeDtypeStruct(shape, dtype) for shape, dtype, s in outs
    ]
    return pl.pallas_call(
        body,
        out_shape=shapes,
        in_specs=[pl.BlockSpec(memory_space=place[s]) for _, s in ins],
        out_specs=[pl.BlockSpec(memory_space=place[s]) for _, _, s in outs],
        scratch_shapes=list(scratch),
        cost_estimate=pl.CostEstimate(flops=flops, bytes_accessed=0, transcendentals=0),
        compiler_params=pltpu.CompilerParams(vmem_limit_bytes=limit * MIB),
    )(*arrays)


def dot(a, b):
    return jnp.dot(a, b, preferred_element_type=F32)


def span(i, size):
    return pl.ds(pl.multiple_of(i * size, size), size)


def rows_in(hbm, held, sems, k, i, size):
    at = span(i, size)
    return pltpu.make_async_copy(hbm.at[at, :], held.at[at, :], sems.at[k, i])


def as_inputs(codes):
    return (codes.astype(F32) * (2.0 / (buckets - 1.0)) - 1.0).astype(BF16)


def decode_body(codes_hbm, w_hbm, hidden_hbm, slope_hbm, sums, codes, weights, hidden, slope, inputs, pre_a, pre_b, totals,
                code_sem, w_sem, out_sem):
    rows, units = hidden.shape
    block, tile = pre_a.shape
    blocks, tiles = rows // block, units // tile
    pres = (pre_a, pre_b)
    part, strip = 32, 256

    def fetch(i):
        at = slice(i * block, (i + 1) * block)
        return pltpu.make_async_copy(codes_hbm.at[at, :], codes.at[at, :], code_sem.at[i])

    def fetch_w(n):
        cols = pl.ds(n * tile, tile)
        return pltpu.make_async_copy(w_hbm.at[:, cols], weights.at[:, cols], w_sem.at[n])

    def put(k, i):
        held, hbm = ((hidden, hidden_hbm), (slope, slope_hbm))[k]
        at = slice(i * block, (i + 1) * block)
        return pltpu.make_async_copy(held.at[at, :], hbm.at[at, :], out_sem.at[k, i])

    fetch(0).start()
    fetch_w(0).start()
    fetch_w(1).start()
    for i in range(1, blocks):
        fetch(i).start()
    totals[...] = jnp.zeros_like(totals)

    def convert(i):
        fetch(i).wait()
        for r in range(block // part):
            at = slice(i * block + r * part, i * block + (r + 1) * part)
            inputs[at, :] = as_inputs(codes[at, :])

    def finish(i, n):
        for c in range(tile // strip):
            cols = slice(n * tile + c * strip, n * tile + (c + 1) * strip)
            first = jnp.zeros((8, strip), F32)
            second = jnp.zeros((8, strip), F32)
            for r in range(block // part):
                at = slice(i * block + r * part, i * block + (r + 1) * part)
                x = pres[n][r * part : (r + 1) * part, c * strip : (c + 1) * strip]
                grown = jnp.exp(jnp.minimum(x, EXP_TOP))
                both = grown * (grown + 2.0)
                inverse = 1.0 / (both + 2.0)
                tangent = both * inverse
                value = x * tangent
                hidden[at, cols] = value
                slope[at, cols] = (tangent + (x * (4.0 * inverse)) * ((grown + grown * grown) * inverse)).astype(BF16)
                first = first + value.reshape(part // 8, 8, strip).sum(0)
                second = second + (value * value).reshape(part // 8, 8, strip).sum(0)
            totals[0:8, cols] += first
            totals[8:16, cols] += second

    convert(0)
    last = None
    for i in range(blocks):
        at = slice(i * block, (i + 1) * block)
        for n in range(tiles):
            if i == 0:
                fetch_w(n).wait()
            if n == tiles - 1 and i + 1 < blocks:
                convert(i + 1)
            pres[n][...] = dot(inputs[at, :], weights[:, n * tile : (n + 1) * tile])
            if last is not None:
                finish(*last)
                if last[1] == tiles - 1:
                    put(0, last[0]).start()
                    put(1, last[0]).start()
            last = (i, n)
    finish(*last)
    put(0, blocks - 1).start()
    put(1, blocks - 1).start()
    first = jnp.sum(totals[0:8, :], 0, keepdims=True)
    second = jnp.sum(totals[8:16, :], 0, keepdims=True)
    for k in range(sums.shape[0]):
        sums[k, 0:1, :] = first
        sums[k, 1:2, :] = second
    for i in range(blocks):
        for k in range(2):
            put(k, i).wait()


def turn_body(codes_hbm, after, turned_hbm, codes, turned, sem, out_sem):
    del after
    rows = codes.shape[0]
    block = LANES
    blocks = rows // block

    def put(i):
        at = span(i, block)
        return pltpu.make_async_copy(turned.at[:, at], turned_hbm.at[:, at], out_sem.at[i])

    for i in range(blocks):
        rows_in(codes_hbm, codes, sem, 0, i, block).start()

    def step(i, carry):
        at = span(i, block)
        rows_in(codes_hbm, codes, sem, 0, i, block).wait()
        for q in range(codes.shape[1] // 256):
            cols = slice(q * 256, (q + 1) * 256)
            turned[cols, at] = as_inputs(codes[at, cols]).T
        put(i).start()
        return carry

    lax.fori_loop(0, blocks, step, 0)
    for i in range(blocks):
        put(i).wait()


def mix_body(after, dense_hbm, mix, w_out, spread_hbm, mixed_t, dense, mixed, spread, sem, out_sem):
    del after
    rows = spread.shape[0]
    block = 64
    deep = dense.shape[1]
    fields = deep // block
    pairs = rows // (2 * block)
    group = rows // 2

    def fetch(i):
        return pltpu.make_async_copy(dense_hbm.at[span(i, deep), :], dense.at[i], sem.at[i])

    def put(i):
        at = slice(i * group, (i + 1) * group)
        return pltpu.make_async_copy(spread.at[at, :], spread_hbm.at[at, :], out_sem.at[i])

    for i in range(2 * pairs):
        fetch(i).start()
    high = mix[...].astype(BF16)
    low = (mix[...] - high.astype(F32)).astype(BF16)
    owner = lax.broadcasted_iota(jnp.int32, (block, deep), 1) // fields
    mine = owner == lax.broadcasted_iota(jnp.int32, (block, deep), 0)
    picks = jnp.concatenate(
        [jnp.where(mine, high.astype(F32), 0.0), jnp.where(mine, low.astype(F32), 0.0)], 0
    ).astype(BF16)

    def step(i, carry):
        fetch(2 * i).wait()
        fetch(2 * i + 1).wait()
        even = dot(picks, dense[2 * i])
        odd = dot(picks, dense[2 * i + 1])
        both = jnp.concatenate([even[:block] + even[block:], odd[:block] + odd[block:]], 0)
        at = span(i, 2 * block)
        mixed_t[:, at] = both.T
        mixed[at, :] = both.astype(BF16)
        return carry

    for g in range(2):
        lax.fori_loop(g * pairs // 2, (g + 1) * pairs // 2, step, 0)
        at = slice(g * group, (g + 1) * group)
        spread[at, :] = lax.dot_general(
            mixed[at, :], w_out[...], (((1,), (1,)), ((), ())), preferred_element_type=F32
        ).astype(BF16)
        put(g).start()
    for g in range(2):
        put(g).wait()


def logit_body(total_rows, arrived, gain, bias, hidden_hbm, spread_hbm, coef, parts, hidden, spread, sem):
    rows, units = hidden.shape
    block = LANES
    blocks = rows // block

    for i in range(blocks):
        rows_in(hidden_hbm, hidden, sem, 0, i, block).start()
        rows_in(spread_hbm, spread, sem, 1, i, block).start()
    stats = jnp.sum(arrived[...], 0)
    mean = stats[0:1] / total_rows
    var = stats[1:2] / total_rows - mean * mean
    inv = lax.rsqrt(var + epsilon)
    coef[0:1, :] = gain[...] * inv
    coef[1:2, :] = bias[...]
    coef[2:3, :] = mean
    coef[3:4, :] = inv

    def step(i, carry):
        at = span(i, block)
        rows_in(hidden_hbm, hidden, sem, 0, i, block).wait()
        rows_in(spread_hbm, spread, sem, 1, i, block).wait()
        total = jnp.zeros((block, LANES), F32)
        for n in range(units // LANES):
            cols = slice(n * LANES, (n + 1) * LANES)
            value = (hidden[at, cols] - coef[2:3, cols]) * coef[0:1, cols] + coef[1:2, cols]
            total = total + value * spread[at, cols].astype(F32)
        line = jnp.sum(total.T, 0, keepdims=True)
        for k in range(parts.shape[0]):
            parts[k, pl.ds(i, 1), :] = line
        return carry

    lax.fori_loop(0, blocks, step, 0)


def column(line):
    return jnp.broadcast_to(line, (LANES, LANES)).T


def two_parts(value):
    high = value.astype(BF16)
    return high, (value - high.astype(F32)).astype(BF16)


def grad_body(total_rows, arrived, labels, hidden_hbm, spread_hbm, coef, mixed_t, grads, packed, hidden, spread,
              normed, weighted, totals, sem):
    rows, units = hidden.shape
    emb = mixed_t.shape[0]
    block = LANES
    blocks = rows // block
    own = packed.shape[0]
    share = units // own
    for i in range(blocks):
        rows_in(hidden_hbm, hidden, sem, 0, i, block).start()
        rows_in(spread_hbm, spread, sem, 1, i, block).start()
    logits = jnp.sum(arrived[...], 0)
    targets = labels[...]
    positive = jnp.maximum(logits, 0.0) + jnp.log1p(jnp.exp(-jnp.abs(logits)))
    loss = jnp.sum(positive - targets * logits, keepdims=True)
    grads[...] = (jax.nn.sigmoid(logits) - targets) * (grad_scale / math.sqrt(total_rows))
    for i in range(blocks):
        at = slice(i * block, (i + 1) * block)
        weighted[:, at] = (mixed_t[:, at] * grads[i : i + 1, :]).astype(BF16)
    totals[...] = jnp.zeros_like(totals)

    def step(i, carry):
        at = span(i, block)
        rows_in(hidden_hbm, hidden, sem, 0, i, block).wait()
        rows_in(spread_hbm, spread, sem, 1, i, block).wait()
        weight = column(grads[pl.ds(i, 1), :])
        for n in range(units // LANES):
            cols = slice(n * LANES, (n + 1) * LANES)
            part = weight * spread[at, cols].astype(F32)
            centred = hidden[at, cols] - coef[2:3, cols]
            normed[at, cols] = (centred * coef[0:1, cols] + coef[1:2, cols]).astype(BF16)
            product = part * centred
            totals[0:8, cols] += part.reshape(block // 8, 8, LANES).sum(0)
            totals[8:16, cols] += product.reshape(block // 8, 8, LANES).sum(0)
        return carry

    lax.fori_loop(0, blocks, step, 0)
    bias = jnp.sum(totals[0:8, :], 0, keepdims=True)
    gain = jnp.sum(totals[8:16, :], 0, keepdims=True) * coef[3:4, :]
    cuts = [slice(q * emb, (q + 1) * emb) for q in range(units // emb)]
    lines = jnp.concatenate([bias[:, c] for c in cuts] + [gain[:, c] for c in cuts], 0)
    spare = [v.astype(F32) for v in two_parts(jnp.broadcast_to(loss, (1, emb)))]
    extra = jnp.concatenate(spare + [jnp.zeros((6, emb), F32)], 0).astype(BF16)
    for p, block_of in enumerate((*two_parts(lines), extra)):
        for k in range(own):
            packed[k, share + 8 * p : share + 8 * p + 8, :] = block_of
    for n in range(units // 512):
        cols = slice(n * 512, (n + 1) * 512)
        out = dot(weighted[...], normed[:, cols]).T.astype(BF16)
        for k in range(512 // share):
            packed[n * (512 // share) + k, 0:share, :] = out[k * share : (k + 1) * share, :]


def ahead_body(chunks, grads, hidden_hbm, spread_hbm, slope_hbm, coef, turned_hbm, terms_hbm, hidden, spread, slope, plain,
               flat, tilted, left, terms, sem, left_sem, out_sem):
    rows, units = hidden.shape
    block = LANES
    blocks = rows // block
    quarter = left.shape[1]
    sub = quarter // 4
    wide = units // 2
    far = [pltpu.make_async_copy(turned_hbm.at[span(chunks[2], quarter), :], left.at[0], left_sem.at[0])]
    for q in range(4):
        at = pl.ds(pl.multiple_of(q * quarter + chunks[6] * sub, sub), sub)
        far.append(pltpu.make_async_copy(turned_hbm.at[at, :], left.at[1, q * sub : (q + 1) * sub, :], left_sem.at[1 + q]))
    for i in range(blocks):
        rows_in(hidden_hbm, hidden, sem, 0, i, block).start()
        rows_in(spread_hbm, spread, sem, 1, i, block).start()
        rows_in(slope_hbm, slope, sem, 2, i, block).start()
    for copy in far:
        copy.start()

    def step(i, carry):
        at = span(i, block)
        rows_in(hidden_hbm, hidden, sem, 0, i, block).wait()
        rows_in(spread_hbm, spread, sem, 1, i, block).wait()
        rows_in(slope_hbm, slope, sem, 2, i, block).wait()
        weight = column(grads[pl.ds(i, 1), :])
        for n in range(units // LANES):
            cols = slice(n * LANES, (n + 1) * LANES)
            factor = coef[0:1, cols] * slope[at, cols].astype(F32)
            flat[at, cols] = factor.astype(BF16)
            plain[at, cols] = (factor * (weight * spread[at, cols].astype(F32))).astype(BF16)
            tilted[at, cols] = (factor * (hidden[at, cols] - coef[2:3, cols])).astype(BF16)
        return carry

    lax.fori_loop(0, blocks, step, 0)
    for copy in far:
        copy.wait()

    def put(k):
        return pltpu.make_async_copy(terms.at[k], terms_hbm.at[k], out_sem.at[k])

    for axis in range(2):
        cols = slice(axis * wide, (axis + 1) * wide)
        for k, right in enumerate((plain, flat, tilted)):
            terms[3 * axis + k] = dot(left[axis], right[:, cols]).astype(BF16)
            put(3 * axis + k).start()
    for k in range(6):
        put(k).wait()


def far_body(total_rows, arrived, coef, terms_hbm, z_hbm, x_hbm, both, grad_gain, grad_bias, loss, piece, terms, held, sem,
             out_sem):
    units = coef.shape[1]
    share, emb = piece.shape
    quarter, wide = terms.shape[1:]
    some = held.shape[1] - quarter

    def get(k):
        return pltpu.make_async_copy(terms_hbm.at[k], terms.at[k], sem.at[k])

    def put(axis):
        return pltpu.make_async_copy(held.at[axis], (z_hbm, x_hbm)[axis], out_sem.at[axis])

    for k in range(6):
        get(k).start()
    count = units // emb

    def stat(p):
        return jnp.sum(arrived[:, share + 8 * p : share + 8 * p + 8, :].astype(F32), 0)

    lines = stat(1) + stat(0)
    for q in range(count):
        cols = slice(q * emb, (q + 1) * emb)
        grad_bias[:, cols] = lines[q : q + 1]
        grad_gain[:, cols] = lines[count + q : count + q + 1]
        both[0:1, cols] = lines[q : q + 1] / total_rows
        both[1:2, cols] = lines[count + q : count + q + 1] * coef[3:4, cols] / total_rows
    loss[...] = jnp.sum(stat(2), 0, keepdims=True)[:, 0:LANES] / total_rows
    piece[...] = jnp.sum(arrived[:, 0:share, :].astype(F32), 0).astype(BF16)
    for axis in range(2):
        first = axis * 2 * some
        for n in range(2):
            held[axis, quarter:, n * 256 : (n + 1) * 256] = piece[first + n * some : first + (n + 1) * some, :]
        for k in range(3):
            get(3 * axis + k).wait()
        for r in range(quarter // LANES):
            at = slice(r * LANES, (r + 1) * LANES)
            for n in range(wide // LANES):
                cols = slice(n * LANES, (n + 1) * LANES)
                here = slice(axis * wide + n * LANES, axis * wide + (n + 1) * LANES)
                value = terms[3 * axis, at, cols].astype(F32) - terms[3 * axis + 1, at, cols].astype(F32) * both[0:1, here]
                value = value - terms[3 * axis + 2, at, cols].astype(F32) * both[1:2, here]
                held[axis, at, cols] = value.astype(BF16)
        put(axis).start()
    for axis in range(2):
        put(axis).wait()


def back_body(grads, hidden_hbm, spread_hbm, slope_hbm, coef, both, grad_pre, hidden, spread, slope, sem):
    rows, units = hidden.shape
    block = LANES
    blocks = rows // block
    for i in range(blocks):
        rows_in(hidden_hbm, hidden, sem, 0, i, block).start()
        rows_in(spread_hbm, spread, sem, 1, i, block).start()
        rows_in(slope_hbm, slope, sem, 2, i, block).start()

    def step(i, carry):
        at = span(i, block)
        rows_in(hidden_hbm, hidden, sem, 0, i, block).wait()
        rows_in(spread_hbm, spread, sem, 1, i, block).wait()
        rows_in(slope_hbm, slope, sem, 2, i, block).wait()
        weight = column(grads[pl.ds(i, 1), :])
        for n in range(units // LANES):
            cols = slice(n * LANES, (n + 1) * LANES)
            inner = weight * spread[at, cols].astype(F32) - both[0:1, cols]
            inner = inner - (hidden[at, cols] - coef[2:3, cols]) * both[1:2, cols]
            grad_pre[at, cols] = (inner * coef[0:1, cols] * slope[at, cols].astype(F32)).astype(BF16)
        return carry

    lax.fori_loop(0, blocks, step, 0)


def product_body(jobs, keep, chunks, turned, grad_pre, piece, after, *refs):
    del after
    count = len(jobs)
    outs, (lines, held, sem) = refs[:count], refs[count:]
    rows = lines.shape[0]
    wide = held.shape[2]
    some = held.shape[1] - rows
    sub = rows // 4

    def put(k):
        return pltpu.make_async_copy(held.at[k], outs[k], sem.at[k])

    for k, (axis, place) in enumerate(jobs):
        c = chunks[place]
        out = outs[k] if keep else held.at[k]
        if axis == "z":
            left = turned[span(c, rows), :]
            base, first = 0, 0
        else:
            for q in range(4):
                at = pl.ds(pl.multiple_of(q * rows + c * sub, sub), sub)
                lines[q * sub : (q + 1) * sub, :] = turned[at, :]
            left = lines[...]
            base, first = wide, 2 * some
        out[0:rows, :] = dot(left, grad_pre[:, base : base + wide]).astype(BF16)
        for n in range(2):
            out[rows:, n * 256 : (n + 1) * 256] = piece[first + n * some : first + (n + 1) * some, :]
        if not keep:
            put(k).start()
    if not keep:
        for k in range(count):
            put(k).wait()


def middle_body(chunk, own, far, up, down, own_out, far_out, up_out, down_out):
    me, was = chunk[0], chunk[1]
    rows = own_out.shape[0]
    full = own.shape[0] - (far_out.shape[0] - rows) // 4
    some = (far_out.shape[0] - rows) // 4
    for step, out in ((2, far_out), (1, up_out), (3, down_out), (0, own_out)):
        at = span(lax.rem(me + step, 4), rows)
        total = (own[at, :].astype(F32) + far[at, :].astype(F32)) + (up[at, :].astype(F32) + down[at, :].astype(F32))
        out[0:rows, :] = total.astype(out.dtype)
        if step:
            for back, came in ((0, own), (2, far), (1, up), (3, down)):
                to = pl.ds(pl.multiple_of(rows + lax.rem(was + 4 - back, 4) * some, some), some)
                out[to, :] = came[full:, :]


def last_body(place, own_a, a0, a2, a1, a3, own_b, b0, b2, b1, b3, hash_hbm, out_hbm, grad_hash, grad_out, sem):
    rows, half = own_a.shape
    some = (a0.shape[0] - rows) // 4
    share = 4 * some
    for kind, pieces in ((0, (a0, a2, a1, a3)), (1, (b0, b2, b1, b3))):
        me = place[1 - kind]
        for back, came in zip((0, 2, 1, 3), pieces):
            there = lax.rem(me + 4 - back, 4)
            for k in range(4):
                owner = k * 4 + there if kind == 0 else there * 4 + k
                for n in range(2):
                    to = pl.ds(pl.multiple_of(owner * share + (2 * kind + n) * some, some), some)
                    at = slice(rows + k * some, rows + (k + 1) * some)
                    grad_out[to, :] = came[at, n * 256 : (n + 1) * 256].astype(F32)
    put_out = pltpu.make_async_copy(grad_out, out_hbm, sem.at[0])
    put_out.start()
    for base, own, came in ((0, own_a, (a2, a1, a3)), (half, own_b, (b2, b1, b3))):
        total = own[...]
        for part in came:
            total = total + part[0:rows, :].astype(F32)
        grad_hash[:, base : base + half] = total
    put_hash = pltpu.make_async_copy(grad_hash, hash_hbm, sem.at[1])
    put_hash.start()
    put_out.wait()
    put_hash.wait()


def on_device(hash_codes, w_hash, norm_gain, norm_bias, w_out, dense_vectors, field_mix, labels):
    rows, codes = hash_codes.shape
    units = w_hash.shape[1]
    fields, emb = dense_vectors.shape[1:]
    dp, mp = lax.axis_size(DP), lax.axis_size(MP)
    total_rows = rows * dp
    lines = rows // LANES
    half = units // 2
    share = units // dp
    some = share // 4
    dma = pltpu.SemaphoreType.DMA
    hidden, slope, sums = call(
        decode_body,
        [(hash_codes, "h"), (w_hash, "h")],
        [((rows, units), F32, "h"), ((rows, units), BF16, "h"), ((dp, 2, units), F32, "v")],
        [
            pltpu.VMEM((rows, codes), jnp.int32),
            pltpu.VMEM((codes, units), BF16),
            pltpu.VMEM((rows, units), F32),
            pltpu.VMEM((rows, units), BF16),
            pltpu.VMEM((rows, codes), BF16),
            pltpu.VMEM((256, units // 2), F32),
            pltpu.VMEM((256, units // 2), F32),
            pltpu.VMEM((16, units), F32),
            dma((rows // 256,)),
            dma((2,)),
            dma((2, rows // 256)),
        ],
        flops=2 * rows * codes * units,
        limit=40,
    )
    arrived = exchange(sums, DP)
    mix_line = jnp.tile(field_mix / math.sqrt(emb), 64).reshape(1, fields * 64)
    spread, mixed_t = call(
        mix_body,
        [(sums, "h"), (dense_vectors.reshape(rows * fields, emb), "h"), (mix_line, "v"), (w_out, "v")],
        [((rows, units), BF16, "h"), ((emb, rows), F32, "v")],
        [
            pltpu.VMEM((rows // 64, fields * 64, emb), BF16),
            pltpu.VMEM((rows, emb), BF16),
            pltpu.VMEM((rows, units), BF16),
            dma((rows // 64,)),
            dma((2,)),
        ],
        flops=8 * rows * units * emb,
        limit=16,
    )
    coef, parts = call(
        functools.partial(logit_body, float(total_rows)),
        [
            (arrived, "v"),
            (norm_gain.reshape(1, units), "v"),
            (norm_bias.reshape(1, units), "v"),
            (hidden, "h"),
            (spread, "h"),
        ],
        [((8, units), F32, "v"), ((mp, lines, LANES), F32, "v")],
        [pltpu.VMEM((rows, units), F32), pltpu.VMEM((rows, units), BF16), dma((2, lines))],
        limit=20,
        flops=4 * rows * units,
    )
    logits = exchange(parts, MP)
    (turned,) = call(
        turn_body,
        [(hash_codes, "h"), (parts, "h")],
        [((codes, rows), BF16, "h")],
        [pltpu.VMEM((rows, codes), jnp.int32), pltpu.VMEM((codes, rows), BF16), dma((1, lines)), dma((lines,))],
        flops=16 * rows * codes * LANES,
        limit=16,
    )
    targets = labels.astype(F32).reshape(lines, LANES)
    grads, packed = call(
        functools.partial(grad_body, float(total_rows)),
        [(logits, "v"), (targets, "v"), (hidden, "h"), (spread, "h"), (coef, "v"), (mixed_t, "v")],
        [((lines, LANES), F32, "v"), ((dp, share + 24, emb), BF16, "v")],
        [
            pltpu.VMEM((rows, units), F32),
            pltpu.VMEM((rows, units), BF16),
            pltpu.VMEM((rows, units), BF16),
            pltpu.VMEM((emb, rows), BF16),
            pltpu.VMEM((16, units), F32),
            dma((2, lines)),
        ],
        limit=24,
        flops=2 * rows * units * emb,
    )
    grad_arrived = exchange(packed, DP)
    here = {axis: lax.axis_index(axis).astype(jnp.int32) for axis in DP}
    chunks = jnp.stack([(here[axis] + step) & 3 for axis in DP for step in range(4)])
    size = (codes // 4 + some, half)
    (terms,) = call(
        ahead_body,
        [
            (chunks, "s"),
            (grads, "v"),
            (hidden, "h"),
            (spread, "h"),
            (slope, "h"),
            (coef, "v"),
            (turned, "h"),
        ],
        [((6, codes // 4, half), BF16, "h")],
        [pltpu.VMEM((rows, units), F32)]
        + [pltpu.VMEM((rows, units), BF16)] * 5
        + [
            pltpu.VMEM((2, codes // 4, rows), BF16),
            pltpu.VMEM((6, codes // 4, half), BF16),
            dma((3, lines)),
            dma((5,)),
            dma((6,)),
        ],
        flops=6 * rows * half * codes,
        limit=30,
    )
    far_z, far_x, both, grad_gain, grad_bias, loss, piece = call(
        functools.partial(far_body, float(total_rows)),
        [(grad_arrived, "v"), (coef, "v"), (terms, "h")],
        [
            (size, BF16, "h"),
            (size, BF16, "h"),
            ((8, units), F32, "p"),
            ((1, units), F32, "v"),
            ((1, units), F32, "v"),
            ((1, LANES), F32, "v"),
            ((share, emb), BF16, "p"),
        ],
        [pltpu.VMEM((6, codes // 4, half), BF16), pltpu.VMEM((2, *size), BF16), dma((6,)), dma((2,))],
        limit=10,
        flops=8 * rows * units,
    )
    (grad_pre,) = call(
        back_body,
        [(grads, "v"), (hidden, "h"), (spread, "h"), (slope, "h"), (coef, "v"), (both, "p")],
        [((rows, units), BF16, "p")],
        [
            pltpu.VMEM((rows, units), F32),
            pltpu.VMEM((rows, units), BF16),
            pltpu.VMEM((rows, units), BF16),
            dma((3, lines)),
        ],
        limit=20,
        flops=8 * rows * units,
    )


    def products(steps, keep, after):
        jobs = [(axis, 4 * DP.index(axis) + step) for step in steps for axis in DP]
        outs = call(
            functools.partial(product_body, jobs, keep),
            [(chunks, "s"), (turned, "p"), (grad_pre, "p"), (piece, "p"), (after, "h")],
            [(size, BF16, "p" if keep else "h")] * len(jobs),
            [pltpu.VMEM((codes // 4, rows), BF16), pltpu.VMEM((1 if keep else len(jobs), *size), BF16), dma((len(jobs),))],
            flops=2 * rows * half * (codes // 4) * len(jobs),
            limit=8,
        )
        return {(axis, place & 3): out for (axis, place), out in zip(jobs, outs)}

    made = {("z", 2): far_z, ("x", 2): far_x}
    made.update(products((1,), False, terms))
    made.update(products((3,), False, made["z", 1]))
    made.update(products((0,), True, made["z", 3]))
    got = {(axis, step): hop(made[axis, step], axis, step) for step in (2, 1, 3) for axis in DP}
    other = {"z": "x", "x": "z"}
    last = []
    for axis in DP:
        own, far, up, down = call(
            middle_body,
            [(jnp.stack([here[other[axis]], here[axis]]), "s"), (made[axis, 0], "p")]
            + [(got[axis, step], "p") for step in (2, 1, 3)],
            [((codes // 16, half), F32, "p")] + [((codes // 16 + 4 * some, half), BF16, "p")] * 3,
            limit=4,
            flops=rows * units,
        )
        last += [own, far] + [hop(v, other[axis], step) for v, step in ((far, 2), (up, 1), (down, 3))]
    grad_hash, grad_out = call(
        last_body,
        [(jnp.stack([here["z"], here["x"]]), "s")] + [(v, "p") for v in last],
        [((codes // 16, units), F32, "h"), ((units, emb), F32, "h")],
        [pltpu.VMEM((codes // 16, units), F32), pltpu.VMEM((units, emb), F32), dma((2,))],
        limit=8,
        flops=rows * units,
    )
    return (grad_hash, grad_gain.reshape(units), grad_bias.reshape(units), grad_out, loss[0, 0])


def solution(mesh):
    split = Mesh(mesh.devices.reshape(4, 4, 4, 2), ("z", "x", "y", "core"))
    return jax.shard_map(
        on_device,
        mesh=split,
        in_specs=(P(DP, None), P(None, MP), P(MP), P(MP), P(MP, None), P(DP, None, None), P(), P(DP)),
        out_specs=(P(DP, MP), P(MP), P(MP), P(MP, None), P()),
        check_vma=False,
    )
```

```python
import functools
import math

import jax
import jax.numpy as jnp
from jax import lax
from jax.experimental import pallas as pl
from jax.experimental.pallas import tpu as pltpu
from jax.sharding import Mesh
from jax.sharding import PartitionSpec as P


DP = ("z", "x")
MP = ("y", "core")
buckets = 32704.0
epsilon = 1e-05
grad_scale = 32.0
EXP_TOP = 20.0
LANES = 128
F32 = jnp.float32
BF16 = jnp.bfloat16
MIB = 1024 * 1024


def hop(value, axis, step):
    count = lax.axis_size(axis)
    return lax.ppermute(value, axis, [(i, (i + step) % count) for i in range(count)])


def exchange(blocks, axes):
    return lax.all_to_all(blocks, axes, 0, 0, tiled=True)


def call(body, ins, outs, scratch=(), flops=0, limit=16):
    place = {"v": pltpu.VMEM, "h": pltpu.HBM, "a": pl.ANY, "s": pltpu.SMEM, "p": pltpu.VMEM}
    held = {"p": pltpu.VMEM, "h": pltpu.HBM}
    arrays = [pltpu.with_memory_space_constraint(a, held[s]) if s in held else a for a, s in ins]
    shapes = [
        held[s](shape, dtype) if s in held else jax.ShapeDtypeStruct(shape, dtype) for shape, dtype, s in outs
    ]
    return pl.pallas_call(
        body,
        out_shape=shapes,
        in_specs=[pl.BlockSpec(memory_space=place[s]) for _, s in ins],
        out_specs=[pl.BlockSpec(memory_space=place[s]) for _, _, s in outs],
        scratch_shapes=list(scratch),
        cost_estimate=pl.CostEstimate(flops=flops, bytes_accessed=0, transcendentals=0),
        compiler_params=pltpu.CompilerParams(vmem_limit_bytes=limit * MIB),
    )(*arrays)


def dot(a, b):
    return jnp.dot(a, b, preferred_element_type=F32)


def span(i, size):
    return pl.ds(pl.multiple_of(i * size, size), size)


def rows_in(hbm, held, sems, k, i, size):
    at = span(i, size)
    return pltpu.make_async_copy(hbm.at[at, :], held.at[at, :], sems.at[k, i])


def as_inputs(codes):
    return (codes.astype(F32) * (2.0 / (buckets - 1.0)) - 1.0).astype(BF16)


def decode_body(codes_hbm, w_hbm, hidden_hbm, slope_hbm, sums, base, codes, weights, hidden, slope, inputs, pre_a, pre_b, kept,
                totals, code_sem, w_sem, out_sem):
    rows, units = hidden.shape
    block, tile = pre_a.shape
    blocks, tiles = rows // block, units // tile
    pres = (pre_a, pre_b)
    part, strip = 32, 256

    def fetch(i):
        at = slice(i * block, (i + 1) * block)
        return pltpu.make_async_copy(codes_hbm.at[at, :], codes.at[at, :], code_sem.at[i])

    def fetch_w(n):
        cols = pl.ds(n * tile, tile)
        return pltpu.make_async_copy(w_hbm.at[:, cols], weights.at[:, cols], w_sem.at[n])

    def put(k, i):
        held, hbm = ((hidden, hidden_hbm), (slope, slope_hbm))[k]
        at = slice(i * block, (i + 1) * block)
        return pltpu.make_async_copy(held.at[at, :], hbm.at[at, :], out_sem.at[k, i])

    fetch(0).start()
    fetch_w(0).start()
    fetch_w(1).start()
    for i in range(1, blocks):
        fetch(i).start()
    totals[...] = jnp.zeros_like(totals)

    def convert(i):
        fetch(i).wait()
        for r in range(block // part):
            at = slice(i * block + r * part, i * block + (r + 1) * part)
            inputs[at, :] = as_inputs(codes[at, :])

    def finish(i, n):
        for c in range(tile // strip):
            cols = slice(n * tile + c * strip, n * tile + (c + 1) * strip)
            first = jnp.zeros((8, strip), F32)
            second = jnp.zeros((8, strip), F32)
            for r in range(block // part):
                at = slice(i * block + r * part, i * block + (r + 1) * part)
                x = pres[n][r * part : (r + 1) * part, c * strip : (c + 1) * strip]
                grown = jnp.exp(jnp.minimum(x, EXP_TOP))
                both = grown * (grown + 2.0)
                inverse = 1.0 / (both + 2.0)
                tangent = both * inverse
                value = x * tangent
                if i == 0:
                    kept[at, cols] = value
                else:
                    hidden[at, cols] = (value - base[:, cols]).astype(BF16)
                slope[at, cols] = (tangent + (x * (4.0 * inverse)) * ((grown + grown * grown) * inverse)).astype(BF16)
                first = first + value.reshape(part // 8, 8, strip).sum(0)
                second = second + (value * value).reshape(part // 8, 8, strip).sum(0)
            if i == 0:
                base[:, cols] = jnp.sum(first, 0, keepdims=True) * (1.0 / block)
                for r in range(block // part):
                    at = slice(r * part, (r + 1) * part)
                    hidden[at, cols] = (kept[at, cols] - base[:, cols]).astype(BF16)
            totals[0:8, cols] += first
            totals[8:16, cols] += second

    convert(0)
    last = None
    for i in range(blocks):
        at = slice(i * block, (i + 1) * block)
        for n in range(tiles):
            if i == 0:
                fetch_w(n).wait()
            if n == tiles - 1 and i + 1 < blocks:
                convert(i + 1)
            pres[n][...] = dot(inputs[at, :], weights[:, n * tile : (n + 1) * tile])
            if last is not None:
                finish(*last)
                if last[1] == tiles - 1:
                    put(0, last[0]).start()
                    put(1, last[0]).start()
            last = (i, n)
    finish(*last)
    put(0, blocks - 1).start()
    put(1, blocks - 1).start()
    first = jnp.sum(totals[0:8, :], 0, keepdims=True)
    second = jnp.sum(totals[8:16, :], 0, keepdims=True)
    for k in range(sums.shape[0]):
        sums[k, 0:1, :] = first
        sums[k, 1:2, :] = second
    for i in range(blocks):
        for k in range(2):
            put(k, i).wait()


def turn_body(codes_hbm, after, turned_hbm, codes, turned, sem, out_sem):
    del after
    rows = codes.shape[0]
    block = LANES
    blocks = rows // block

    def put(i):
        at = span(i, block)
        return pltpu.make_async_copy(turned.at[:, at], turned_hbm.at[:, at], out_sem.at[i])

    for i in range(blocks):
        rows_in(codes_hbm, codes, sem, 0, i, block).start()

    def step(i, carry):
        at = span(i, block)
        rows_in(codes_hbm, codes, sem, 0, i, block).wait()
        for q in range(codes.shape[1] // 256):
            cols = slice(q * 256, (q + 1) * 256)
            turned[cols, at] = as_inputs(codes[at, cols]).T
        put(i).start()
        return carry

    lax.fori_loop(0, blocks, step, 0)
    for i in range(blocks):
        put(i).wait()


def mix_body(after, dense_hbm, mix, w_out, spread_hbm, mixed_t, dense, mixed, spread, sem, out_sem):
    del after
    rows = spread.shape[0]
    block = 64
    deep = dense.shape[1]
    fields = deep // block
    pairs = rows // (2 * block)
    group = rows // 2

    def fetch(i):
        return pltpu.make_async_copy(dense_hbm.at[span(i, deep), :], dense.at[i], sem.at[i])

    def put(i):
        at = slice(i * group, (i + 1) * group)
        return pltpu.make_async_copy(spread.at[at, :], spread_hbm.at[at, :], out_sem.at[i])

    for i in range(2 * pairs):
        fetch(i).start()
    high = mix[...].astype(BF16)
    low = (mix[...] - high.astype(F32)).astype(BF16)
    owner = lax.broadcasted_iota(jnp.int32, (block, deep), 1) // fields
    mine = owner == lax.broadcasted_iota(jnp.int32, (block, deep), 0)
    picks = jnp.concatenate(
        [jnp.where(mine, high.astype(F32), 0.0), jnp.where(mine, low.astype(F32), 0.0)], 0
    ).astype(BF16)

    def step(i, carry):
        fetch(2 * i).wait()
        fetch(2 * i + 1).wait()
        even = dot(picks, dense[2 * i])
        odd = dot(picks, dense[2 * i + 1])
        both = jnp.concatenate([even[:block] + even[block:], odd[:block] + odd[block:]], 0)
        at = span(i, 2 * block)
        mixed_t[:, at] = both.T
        mixed[at, :] = both.astype(BF16)
        return carry

    for g in range(2):
        lax.fori_loop(g * pairs // 2, (g + 1) * pairs // 2, step, 0)
        at = slice(g * group, (g + 1) * group)
        spread[at, :] = lax.dot_general(
            mixed[at, :], w_out[...], (((1,), (1,)), ((), ())), preferred_element_type=F32
        ).astype(BF16)
        put(g).start()
    for g in range(2):
        put(g).wait()


def logit_body(total_rows, arrived, gain, bias, base, hidden_hbm, spread_hbm, coef, parts, hidden, spread, sem):
    rows, units = hidden.shape
    block = LANES
    blocks = rows // block

    for i in range(blocks):
        rows_in(hidden_hbm, hidden, sem, 0, i, block).start()
        rows_in(spread_hbm, spread, sem, 1, i, block).start()
    stats = jnp.sum(arrived[...], 0)
    mean = stats[0:1] / total_rows
    var = stats[1:2] / total_rows - mean * mean
    inv = lax.rsqrt(var + epsilon)
    coef[0:1, :] = gain[...] * inv
    coef[1:2, :] = bias[...]
    coef[2:3, :] = mean - base[...]
    coef[3:4, :] = inv

    def step(i, carry):
        at = span(i, block)
        rows_in(hidden_hbm, hidden, sem, 0, i, block).wait()
        rows_in(spread_hbm, spread, sem, 1, i, block).wait()
        total = jnp.zeros((block, LANES), F32)
        for n in range(units // LANES):
            cols = slice(n * LANES, (n + 1) * LANES)
            value = (hidden[at, cols].astype(F32) - coef[2:3, cols]) * coef[0:1, cols] + coef[1:2, cols]
            total = total + value * spread[at, cols].astype(F32)
        line = jnp.sum(total.T, 0, keepdims=True)
        for k in range(parts.shape[0]):
            parts[k, pl.ds(i, 1), :] = line
        return carry

    lax.fori_loop(0, blocks, step, 0)


def column(line):
    return jnp.broadcast_to(line, (LANES, LANES)).T


def two_parts(value):
    high = value.astype(BF16)
    return high, (value - high.astype(F32)).astype(BF16)


def grad_body(total_rows, arrived, labels, hidden_hbm, spread_hbm, coef, mixed_t, grads, packed, hidden, spread,
              normed, weighted, totals, sem):
    rows, units = hidden.shape
    emb = mixed_t.shape[0]
    block = LANES
    blocks = rows // block
    own = packed.shape[0]
    share = units // own
    for i in range(blocks):
        rows_in(hidden_hbm, hidden, sem, 0, i, block).start()
        rows_in(spread_hbm, spread, sem, 1, i, block).start()
    logits = jnp.sum(arrived[...], 0)
    targets = labels[...]
    positive = jnp.maximum(logits, 0.0) + jnp.log1p(jnp.exp(-jnp.abs(logits)))
    loss = jnp.sum(positive - targets * logits, keepdims=True)
    grads[...] = (jax.nn.sigmoid(logits) - targets) * (grad_scale / math.sqrt(total_rows))
    for i in range(blocks):
        at = slice(i * block, (i + 1) * block)
        weighted[:, at] = (mixed_t[:, at] * grads[i : i + 1, :]).astype(BF16)
    totals[...] = jnp.zeros_like(totals)

    def step(i, carry):
        at = span(i, block)
        rows_in(hidden_hbm, hidden, sem, 0, i, block).wait()
        rows_in(spread_hbm, spread, sem, 1, i, block).wait()
        weight = column(grads[pl.ds(i, 1), :])
        for n in range(units // LANES):
            cols = slice(n * LANES, (n + 1) * LANES)
            part = weight * spread[at, cols].astype(F32)
            centred = hidden[at, cols].astype(F32) - coef[2:3, cols]
            normed[at, cols] = (centred * coef[0:1, cols] + coef[1:2, cols]).astype(BF16)
            product = part * centred
            totals[0:8, cols] += part.reshape(block // 8, 8, LANES).sum(0)
            totals[8:16, cols] += product.reshape(block // 8, 8, LANES).sum(0)
        return carry

    lax.fori_loop(0, blocks, step, 0)
    bias = jnp.sum(totals[0:8, :], 0, keepdims=True)
    gain = jnp.sum(totals[8:16, :], 0, keepdims=True) * coef[3:4, :]
    cuts = [slice(q * emb, (q + 1) * emb) for q in range(units // emb)]
    lines = jnp.concatenate([bias[:, c] for c in cuts] + [gain[:, c] for c in cuts], 0)
    spare = [v.astype(F32) for v in two_parts(jnp.broadcast_to(loss, (1, emb)))]
    extra = jnp.concatenate(spare + [jnp.zeros((6, emb), F32)], 0).astype(BF16)
    for p, block_of in enumerate((*two_parts(lines), extra)):
        for k in range(own):
            packed[k, share + 8 * p : share + 8 * p + 8, :] = block_of
    for n in range(units // 512):
        cols = slice(n * 512, (n + 1) * 512)
        out = dot(weighted[...], normed[:, cols]).T.astype(BF16)
        for k in range(512 // share):
            packed[n * (512 // share) + k, 0:share, :] = out[k * share : (k + 1) * share, :]


def lefts(turned_hbm, left, sem, z_chunk, x_chunk):
    quarter = left.shape[1]
    sub = quarter // 4
    copies = [pltpu.make_async_copy(turned_hbm.at[span(z_chunk, quarter), :], left.at[0], sem.at[0])]
    for q in range(4):
        at = pl.ds(pl.multiple_of(q * quarter + x_chunk * sub, sub), sub)
        copies.append(pltpu.make_async_copy(turned_hbm.at[at, :], left.at[1, q * sub : (q + 1) * sub, :], sem.at[1 + q]))
    return copies


def ahead_body(chunks, grads, hidden_hbm, spread_hbm, slope_hbm, coef, turned_hbm, terms_hbm, hidden, spread, slope, plain,
               flat, tilted, left, terms, sem, left_sem, out_sem):
    rows, units = hidden.shape
    block = LANES
    blocks = rows // block
    wide = units // 2
    far = lefts(turned_hbm, left, left_sem, chunks[2], chunks[6])
    for i in range(blocks):
        rows_in(hidden_hbm, hidden, sem, 0, i, block).start()
        rows_in(spread_hbm, spread, sem, 1, i, block).start()
        rows_in(slope_hbm, slope, sem, 2, i, block).start()
    for copy in far:
        copy.start()

    def step(i, carry):
        at = span(i, block)
        rows_in(hidden_hbm, hidden, sem, 0, i, block).wait()
        rows_in(spread_hbm, spread, sem, 1, i, block).wait()
        rows_in(slope_hbm, slope, sem, 2, i, block).wait()
        weight = column(grads[pl.ds(i, 1), :])
        for n in range(units // LANES):
            cols = slice(n * LANES, (n + 1) * LANES)
            factor = coef[0:1, cols] * slope[at, cols].astype(F32)
            flat[at, cols] = factor.astype(BF16)
            plain[at, cols] = (factor * (weight * spread[at, cols].astype(F32))).astype(BF16)
            tilted[at, cols] = (factor * (hidden[at, cols].astype(F32) - coef[2:3, cols])).astype(BF16)
        return carry

    lax.fori_loop(0, blocks, step, 0)
    for copy in far:
        copy.wait()

    def put(k):
        return pltpu.make_async_copy(terms.at[k], terms_hbm.at[k], out_sem.at[k])

    for axis in range(2):
        cols = slice(axis * wide, (axis + 1) * wide)
        for k, right in enumerate((plain, flat, tilted)):
            terms[3 * axis + k] = dot(left[axis], right[:, cols]).astype(BF16)
            put(3 * axis + k).start()
    for k in range(6):
        put(k).wait()


def lay_piece(message, piece, below):
    half = piece.shape[0] // 2
    wide = piece.shape[1]
    for n in range(2):
        message[below:, n * wide : (n + 1) * wide] = piece[n * half : (n + 1) * half, :]


def far_body(total_rows, arrived, coef, terms_hbm, z_hbm, x_hbm, both, piece, terms, held_z, held_x, sem, out_sem):
    units = coef.shape[1]
    share, emb = piece.shape
    quarter, wide = terms.shape[1:]
    held = (held_z, held_x)

    def get(k):
        return pltpu.make_async_copy(terms_hbm.at[k], terms.at[k], sem.at[k])

    def put(axis):
        return pltpu.make_async_copy(held[axis], (z_hbm, x_hbm)[axis], out_sem.at[axis])

    for k in range(6):
        get(k).start()
    count = units // emb

    def stat(p):
        return jnp.sum(arrived[:, share + 8 * p : share + 8 * p + 8, :].astype(F32), 0)

    lines = stat(1) + stat(0)
    for q in range(count):
        cols = slice(q * emb, (q + 1) * emb)
        both[2:3, cols] = lines[q : q + 1]
        both[3:4, cols] = lines[count + q : count + q + 1]
        both[0:1, cols] = lines[q : q + 1] / total_rows
        both[1:2, cols] = lines[count + q : count + q + 1] * coef[3:4, cols] / total_rows
    both[4:5, 0:emb] = jnp.sum(stat(2), 0, keepdims=True) / total_rows
    piece[...] = jnp.sum(arrived[:, 0:share, :].astype(F32), 0).astype(BF16)
    for axis in range(2):
        if axis == 1:
            lay_piece(held_x, piece, quarter)
        for k in range(3):
            get(3 * axis + k).wait()
        for r in range(quarter // LANES):
            at = slice(r * LANES, (r + 1) * LANES)
            for n in range(wide // LANES):
                cols = slice(n * LANES, (n + 1) * LANES)
                here = slice(axis * wide + n * LANES, axis * wide + (n + 1) * LANES)
                value = terms[3 * axis, at, cols].astype(F32) - terms[3 * axis + 1, at, cols].astype(F32) * both[0:1, here]
                value = value - terms[3 * axis + 2, at, cols].astype(F32) * both[1:2, here]
                held[axis][at, cols] = value.astype(BF16)
        put(axis).start()
    for axis in range(2):
        put(axis).wait()


def product(axis, chunk, turned, grad_pre, piece, lines, out):
    rows, wide = lines.shape[0], out.shape[1]
    sub = rows // 4
    if axis == 0:
        left = turned[span(chunk, rows), :]
    else:
        for q in range(4):
            at = pl.ds(pl.multiple_of(q * rows + chunk * sub, sub), sub)
            lines[q * sub : (q + 1) * sub, :] = turned[at, :]
        left = lines[...]
        lay_piece(out, piece, rows)
    out[0:rows, :] = dot(left, grad_pre[:, axis * wide : (axis + 1) * wide]).astype(BF16)


def near_body(chunks, grads, hidden_hbm, spread_hbm, slope_hbm, coef, both, turned_hbm, piece, grad_pre, grad_gain, grad_bias,
              loss, z1_hbm, x1_hbm, z3_hbm, x3_hbm, hidden, spread, slope, turned, lines, z1, x1, z3, x3, sem,
              turned_sem, out_sem):
    rows, units = hidden.shape
    block = LANES
    blocks = rows // block
    parts = turned_sem.shape[0]

    def turn_in(i):
        at = span(i, turned.shape[0] // parts)
        return pltpu.make_async_copy(turned_hbm.at[at, :], turned.at[at, :], turned_sem.at[i])

    for i in range(blocks):
        rows_in(hidden_hbm, hidden, sem, 0, i, block).start()
        rows_in(spread_hbm, spread, sem, 1, i, block).start()
        rows_in(slope_hbm, slope, sem, 2, i, block).start()
    for i in range(parts):
        turn_in(i).start()
    grad_bias[...] = both[2:3, :]
    grad_gain[...] = both[3:4, :]
    loss[...] = both[4:5, 0:LANES]

    def step(i, carry):
        at = span(i, block)
        rows_in(hidden_hbm, hidden, sem, 0, i, block).wait()
        rows_in(spread_hbm, spread, sem, 1, i, block).wait()
        rows_in(slope_hbm, slope, sem, 2, i, block).wait()
        weight = column(grads[pl.ds(i, 1), :])
        for n in range(units // LANES):
            cols = slice(n * LANES, (n + 1) * LANES)
            inner = weight * spread[at, cols].astype(F32) - both[0:1, cols]
            inner = inner - (hidden[at, cols].astype(F32) - coef[2:3, cols]) * both[1:2, cols]
            grad_pre[at, cols] = (inner * coef[0:1, cols] * slope[at, cols].astype(F32)).astype(BF16)
        return carry

    lax.fori_loop(0, blocks, step, 0)
    for i in range(parts):
        turn_in(i).wait()
    jobs = ((0, 1, z1, z1_hbm), (1, 1, x1, x1_hbm), (0, 3, z3, z3_hbm), (1, 3, x3, x3_hbm))

    def put(k):
        return pltpu.make_async_copy(jobs[k][2], jobs[k][3], out_sem.at[k])

    for k, (axis, step_on, held, _) in enumerate(jobs):
        product(axis, chunks[4 * axis + step_on], turned, grad_pre, piece, lines, held)
        put(k).start()
    for k in range(len(jobs)):
        put(k).wait()


def own_body(chunks, turned_hbm, grad_pre, piece, after, z0, x0, left, sem):
    del after
    copies = lefts(turned_hbm, left, sem, chunks[0], chunks[4])
    for copy in copies:
        copy.start()
    rows, wide = z0.shape
    lay_piece(x0, piece, rows)
    for copy in copies:
        copy.wait()
    for axis, out in ((0, z0), (1, x0)):
        out[0:rows, :] = dot(left[axis], grad_pre[:, axis * wide : (axis + 1) * wide]).astype(BF16)


def middle_body(chunk, own, far, up, down, own_out, far_out, up_out, down_out):
    me, was = chunk[0], chunk[1]
    rows = own_out.shape[0]
    full = own.shape[0] - (far_out.shape[0] - rows) // 4
    some = (far_out.shape[0] - rows) // 4
    for step, out in ((2, far_out), (1, up_out), (3, down_out), (0, own_out)):
        at = span(lax.rem(me + step, 4), rows)
        total = (own[at, :].astype(F32) + far[at, :].astype(F32)) + (up[at, :].astype(F32) + down[at, :].astype(F32))
        out[0:rows, :] = total.astype(out.dtype)
        if step and some:
            for back, came in ((0, own), (2, far), (1, up), (3, down)):
                to = pl.ds(pl.multiple_of(rows + lax.rem(was + 4 - back, 4) * some, some), some)
                out[to, :] = came[full:, :]


def last_body(place, own_a, a2, a1, a3, own_b, b0, b2, b1, b3, hash_hbm, out_hbm, grad_hash, grad_out, sem):
    rows, half = own_a.shape
    some = (b0.shape[0] - rows) // 4
    share = 2 * some
    emb = grad_out.shape[1]
    for back, came in zip((0, 2, 1, 3), (b0, b2, b1, b3)):
        there = lax.rem(place[0] + 4 - back, 4)
        for k in range(4):
            for n in range(2):
                to = pl.ds(pl.multiple_of((there * 4 + k) * share + n * some, some), some)
                at = slice(rows + k * some, rows + (k + 1) * some)
                grad_out[to, :] = came[at, n * emb : (n + 1) * emb].astype(F32)
    put_out = pltpu.make_async_copy(grad_out, out_hbm, sem.at[0])
    put_out.start()
    for base, own, came in ((0, own_a, (a2, a1, a3)), (half, own_b, (b2, b1, b3))):
        total = own[...]
        for part in came:
            total = total + part[0:rows, :].astype(F32)
        grad_hash[:, base : base + half] = total
    put_hash = pltpu.make_async_copy(grad_hash, hash_hbm, sem.at[1])
    put_hash.start()
    put_out.wait()
    put_hash.wait()


def on_device(hash_codes, w_hash, norm_gain, norm_bias, w_out, dense_vectors, field_mix, labels):
    rows, codes = hash_codes.shape
    units = w_hash.shape[1]
    fields, emb = dense_vectors.shape[1:]
    dp, mp = lax.axis_size(DP), lax.axis_size(MP)
    total_rows = rows * dp
    lines = rows // LANES
    half = units // 2
    share = units // dp
    some = share // 4
    dma = pltpu.SemaphoreType.DMA
    hidden, slope, sums, base = call(
        decode_body,
        [(hash_codes, "h"), (w_hash, "h")],
        [((rows, units), BF16, "h"), ((rows, units), BF16, "h"), ((dp, 2, units), F32, "v"), ((1, units), F32, "v")],
        [
            pltpu.VMEM((rows, codes), jnp.int32),
            pltpu.VMEM((codes, units), BF16),
            pltpu.VMEM((rows, units), BF16),
            pltpu.VMEM((rows, units), BF16),
            pltpu.VMEM((rows, codes), BF16),
            pltpu.VMEM((256, units // 2), F32),
            pltpu.VMEM((256, units // 2), F32),
            pltpu.VMEM((256, units), F32),
            pltpu.VMEM((16, units), F32),
            dma((rows // 256,)),
            dma((2,)),
            dma((2, rows // 256)),
        ],
        flops=2 * rows * codes * units,
        limit=40,
    )
    arrived = exchange(sums, DP)
    mix_line = jnp.tile(field_mix / math.sqrt(emb), 64).reshape(1, fields * 64)
    spread, mixed_t = call(
        mix_body,
        [(sums, "h"), (dense_vectors.reshape(rows * fields, emb), "h"), (mix_line, "v"), (w_out, "v")],
        [((rows, units), BF16, "h"), ((emb, rows), F32, "v")],
        [
            pltpu.VMEM((rows // 64, fields * 64, emb), BF16),
            pltpu.VMEM((rows, emb), BF16),
            pltpu.VMEM((rows, units), BF16),
            dma((rows // 64,)),
            dma((2,)),
        ],
        flops=8 * rows * units * emb,
        limit=16,
    )
    coef, parts = call(
        functools.partial(logit_body, float(total_rows)),
        [
            (arrived, "v"),
            (norm_gain.reshape(1, units), "v"),
            (norm_bias.reshape(1, units), "v"),
            (base, "v"),
            (hidden, "h"),
            (spread, "h"),
        ],
        [((8, units), F32, "v"), ((mp, lines, LANES), F32, "v")],
        [pltpu.VMEM((rows, units), BF16), pltpu.VMEM((rows, units), BF16), dma((2, lines))],
        limit=20,
        flops=4 * rows * units,
    )
    logits = exchange(parts, MP)
    (turned,) = call(
        turn_body,
        [(hash_codes, "h"), (parts, "h")],
        [((codes, rows), BF16, "h")],
        [pltpu.VMEM((rows, codes), jnp.int32), pltpu.VMEM((codes, rows), BF16), dma((1, lines)), dma((lines,))],
        flops=16 * rows * codes * LANES,
        limit=16,
    )
    targets = labels.astype(F32).reshape(lines, LANES)
    grads, packed = call(
        functools.partial(grad_body, float(total_rows)),
        [(logits, "v"), (targets, "v"), (hidden, "h"), (spread, "h"), (coef, "v"), (mixed_t, "v")],
        [((lines, LANES), F32, "v"), ((dp, share + 24, emb), BF16, "v")],
        [
            pltpu.VMEM((rows, units), BF16),
            pltpu.VMEM((rows, units), BF16),
            pltpu.VMEM((rows, units), BF16),
            pltpu.VMEM((emb, rows), BF16),
            pltpu.VMEM((16, units), F32),
            dma((2, lines)),
        ],
        limit=24,
        flops=2 * rows * units * emb,
    )
    grad_arrived = exchange(packed, DP)
    here = {axis: lax.axis_index(axis).astype(jnp.int32) for axis in DP}
    chunks = jnp.stack([(here[axis] + step) & 3 for axis in DP for step in range(4)])
    sizes = ((codes // 4, half), (codes // 4 + 2 * some, half))
    (terms,) = call(
        ahead_body,
        [
            (chunks, "s"),
            (grads, "v"),
            (hidden, "h"),
            (spread, "h"),
            (slope, "h"),
            (coef, "v"),
            (turned, "h"),
        ],
        [((6, codes // 4, half), BF16, "h")],
        [pltpu.VMEM((rows, units), BF16)] * 6
        + [
            pltpu.VMEM((2, codes // 4, rows), BF16),
            pltpu.VMEM((6, codes // 4, half), BF16),
            dma((3, lines)),
            dma((5,)),
            dma((6,)),
        ],
        flops=6 * rows * half * codes,
        limit=30,
    )
    far_z, far_x, both, piece = call(
        functools.partial(far_body, float(total_rows)),
        [(grad_arrived, "v"), (coef, "v"), (terms, "h")],
        [
            (sizes[0], BF16, "h"),
            (sizes[1], BF16, "h"),
            ((8, units), F32, "p"),
            ((share, emb), BF16, "p"),
        ],
        [pltpu.VMEM((6, codes // 4, half), BF16)] + [pltpu.VMEM(size, BF16) for size in sizes] + [dma((6,)), dma((2,))],
        limit=10,
        flops=8 * rows * units,
    )
    near = call(
        near_body,
        [
            (chunks, "s"),
            (grads, "v"),
            (hidden, "h"),
            (spread, "h"),
            (slope, "h"),
            (coef, "v"),
            (both, "p"),
            (turned, "h"),
            (piece, "p"),
        ],
        [((rows, units), BF16, "p"), ((1, units), F32, "v"), ((1, units), F32, "v"), ((1, LANES), F32, "v")]
        + [(size, BF16, "h") for size in sizes * 2],
        [pltpu.VMEM((rows, units), BF16)] * 3
        + [pltpu.VMEM((codes, rows), BF16), pltpu.VMEM((codes // 4, rows), BF16)]
        + [pltpu.VMEM(size, BF16) for size in sizes * 2]
        + [dma((3, lines)), dma((4,)), dma((4,))],
        limit=20,
        flops=2 * rows * half * codes,
    )
    grad_pre, grad_gain, grad_bias, loss = near[:4]
    own_z, own_x = call(
        own_body,
        [(chunks, "s"), (turned, "h"), (grad_pre, "p"), (piece, "p"), (near[7], "h")],
        [(size, BF16, "p") for size in sizes],
        [pltpu.VMEM((2, codes // 4, rows), BF16), dma((5,))],
        limit=6,
        flops=rows * half * codes,
    )
    made = {("z", 2): far_z, ("x", 2): far_x, ("z", 0): own_z, ("x", 0): own_x}
    made.update(zip((("z", 1), ("x", 1), ("z", 3), ("x", 3)), near[4:]))
    got = {(axis, step): hop(made[axis, step], axis, step) for step in (2, 1, 3) for axis in DP}
    other = {"z": "x", "x": "z"}
    last = []
    for axis in DP:
        own, far, up, down = call(
            middle_body,
            [(jnp.stack([here[other[axis]], here[axis]]), "s"), (made[axis, 0], "p")]
            + [(got[axis, step], "p") for step in (2, 1, 3)],
            [((codes // 16, half), F32, "p")] + [((codes // 16 + 8 * some * (axis == "x"), half), BF16, "p")] * 3,
            limit=4,
            flops=rows * units,
        )
        last += [own] + [far] * (axis == "x") + [hop(v, other[axis], step) for v, step in ((far, 2), (up, 1), (down, 3))]
    grad_hash, grad_out = call(
        last_body,
        [(jnp.stack([here["z"], here["x"]]), "s")] + [(v, "p") for v in last],
        [((codes // 16, units), F32, "h"), ((units, emb), F32, "h")],
        [pltpu.VMEM((codes // 16, units), F32), pltpu.VMEM((units, emb), F32), dma((2,))],
        limit=8,
        flops=rows * units,
    )
    return (grad_hash, grad_gain.reshape(units), grad_bias.reshape(units), grad_out, loss[0, 0])


def solution(mesh):
    split = Mesh(mesh.devices.reshape(4, 4, 4, 2), ("z", "x", "y", "core"))
    return jax.shard_map(
        on_device,
        mesh=split,
        in_specs=(P(DP, None), P(None, MP), P(MP), P(MP), P(MP, None), P(DP, None, None), P(), P(DP)),
        out_specs=(P(DP, MP), P(MP), P(MP), P(MP, None), P()),
        check_vma=False,
    )
```

```python
import functools
import math

import jax
import jax.numpy as jnp
from jax import lax
from jax.experimental import pallas as pl
from jax.experimental.pallas import tpu as pltpu
from jax.sharding import Mesh
from jax.sharding import PartitionSpec as P


DP = ("z", "x")
MP = ("y", "core")
buckets = 32704.0
epsilon = 1e-05
grad_scale = 32.0
EXP_TOP = 20.0
LANES = 128
F32 = jnp.float32
BF16 = jnp.bfloat16
MIB = 1024 * 1024


def hop(value, axis, step):
    count = lax.axis_size(axis)
    return lax.ppermute(value, axis, [(i, (i + step) % count) for i in range(count)])


def exchange(blocks, axes):
    return lax.all_to_all(blocks, axes, 0, 0, tiled=True)


def call(body, ins, outs, scratch=(), flops=0, limit=16):
    place = {"v": pltpu.VMEM, "h": pltpu.HBM, "a": pl.ANY, "s": pltpu.SMEM, "p": pltpu.VMEM}
    held = {"p": pltpu.VMEM, "h": pltpu.HBM}
    arrays = [pltpu.with_memory_space_constraint(a, held[s]) if s in held else a for a, s in ins]
    shapes = [
        held[s](shape, dtype) if s in held else jax.ShapeDtypeStruct(shape, dtype) for shape, dtype, s in outs
    ]
    return pl.pallas_call(
        body,
        out_shape=shapes,
        in_specs=[pl.BlockSpec(memory_space=place[s]) for _, s in ins],
        out_specs=[pl.BlockSpec(memory_space=place[s]) for _, _, s in outs],
        scratch_shapes=list(scratch),
        cost_estimate=pl.CostEstimate(flops=flops, bytes_accessed=0, transcendentals=0),
        compiler_params=pltpu.CompilerParams(vmem_limit_bytes=limit * MIB),
    )(*arrays)


def dot(a, b):
    return jnp.dot(a, b, preferred_element_type=F32)


def span(i, size):
    return pl.ds(pl.multiple_of(i * size, size), size)


def rows_in(hbm, held, sems, k, i, size):
    at = span(i, size)
    return pltpu.make_async_copy(hbm.at[at, :], held.at[at, :], sems.at[k, i])


def as_inputs(codes):
    return (codes.astype(F32) * (2.0 / (buckets - 1.0)) - 1.0).astype(BF16)


def decode_body(codes_hbm, w_hbm, hidden_hbm, slope_hbm, sums_hbm, base, codes, weights, hidden, slope, inputs, pre_a, pre_b, kept,
                totals, sums, code_sem, w_sem, out_sem, sum_sem):
    rows, units = hidden.shape
    block, tile = pre_a.shape
    blocks, tiles = rows // block, units // tile
    pres = (pre_a, pre_b)
    part, strip = 32, 256

    def fetch(i):
        at = slice(i * block, (i + 1) * block)
        return pltpu.make_async_copy(codes_hbm.at[at, :], codes.at[at, :], code_sem.at[i])

    def fetch_w(n):
        cols = pl.ds(n * tile, tile)
        return pltpu.make_async_copy(w_hbm.at[:, cols], weights.at[:, cols], w_sem.at[n])

    def put(k, i):
        held, hbm = ((hidden, hidden_hbm), (slope, slope_hbm))[k]
        at = slice(i * block, (i + 1) * block)
        return pltpu.make_async_copy(held.at[at, :], hbm.at[at, :], out_sem.at[k, i])

    fetch(0).start()
    fetch_w(0).start()
    fetch_w(1).start()
    for i in range(1, blocks):
        fetch(i).start()
    totals[...] = jnp.zeros_like(totals)

    def convert(i):
        fetch(i).wait()
        for r in range(block // part):
            at = slice(i * block + r * part, i * block + (r + 1) * part)
            inputs[at, :] = as_inputs(codes[at, :])

    def finish(i, n):
        for c in range(tile // strip):
            cols = slice(n * tile + c * strip, n * tile + (c + 1) * strip)
            first = jnp.zeros((8, strip), F32)
            second = jnp.zeros((8, strip), F32)
            for r in range(block // part):
                at = slice(i * block + r * part, i * block + (r + 1) * part)
                x = pres[n][r * part : (r + 1) * part, c * strip : (c + 1) * strip]
                grown = jnp.exp(jnp.minimum(x, EXP_TOP))
                both = grown * (grown + 2.0)
                inverse = 1.0 / (both + 2.0)
                tangent = both * inverse
                value = x * tangent
                if i == 0:
                    kept[at, cols] = value
                else:
                    hidden[at, cols] = (value - base[:, cols]).astype(BF16)
                slope[at, cols] = (tangent + (x * (4.0 * inverse)) * ((grown + grown * grown) * inverse)).astype(BF16)
                first = first + value.reshape(part // 8, 8, strip).sum(0)
                second = second + (value * value).reshape(part // 8, 8, strip).sum(0)
            if i == 0:
                base[:, cols] = jnp.sum(first, 0, keepdims=True) * (1.0 / block)
                for r in range(block // part):
                    at = slice(r * part, (r + 1) * part)
                    hidden[at, cols] = (kept[at, cols] - base[:, cols]).astype(BF16)
            totals[0:8, cols] += first
            totals[8:16, cols] += second

    convert(0)
    last = None
    for i in range(blocks):
        at = slice(i * block, (i + 1) * block)
        for n in range(tiles):
            if i == 0:
                fetch_w(n).wait()
            if n == tiles - 1 and i + 1 < blocks:
                convert(i + 1)
            pres[n][...] = dot(inputs[at, :], weights[:, n * tile : (n + 1) * tile])
            if last is not None:
                finish(*last)
                if last[1] == tiles - 1:
                    put(0, last[0]).start()
                    put(1, last[0]).start()
            last = (i, n)
    finish(*last)
    put(0, blocks - 1).start()
    put(1, blocks - 1).start()
    first = jnp.sum(totals[0:8, :], 0, keepdims=True)
    second = jnp.sum(totals[8:16, :], 0, keepdims=True)
    for k in range(sums.shape[0]):
        sums[k, 0:1, :] = first
        sums[k, 1:2, :] = second
    put_sums = pltpu.make_async_copy(sums, sums_hbm, sum_sem.at[0])
    put_sums.start()
    put_sums.wait()
    for i in range(blocks):
        for k in range(2):
            put(k, i).wait()


def turn_body(codes_hbm, after, turned_hbm, codes, turned, sem, out_sem):
    del after
    rows = codes.shape[0]
    block = LANES
    blocks = rows // block

    def put(i):
        at = span(i, block)
        return pltpu.make_async_copy(turned.at[:, at], turned_hbm.at[:, at], out_sem.at[i])

    for i in range(blocks):
        rows_in(codes_hbm, codes, sem, 0, i, block).start()

    def step(i, carry):
        at = span(i, block)
        rows_in(codes_hbm, codes, sem, 0, i, block).wait()
        for q in range(codes.shape[1] // 256):
            cols = slice(q * 256, (q + 1) * 256)
            turned[cols, at] = as_inputs(codes[at, cols]).T
        put(i).start()
        return carry

    lax.fori_loop(0, blocks, step, 0)
    for i in range(blocks):
        put(i).wait()


def mix_body(after, dense_hbm, mix, w_out, spread_hbm, mixed_t, dense, mixed, spread, sem, out_sem):
    del after
    rows = spread.shape[0]
    block = 64
    deep = dense.shape[1]
    fields = deep // block
    pairs = rows // (2 * block)
    group = rows // 2

    def fetch(i):
        return pltpu.make_async_copy(dense_hbm.at[span(i, deep), :], dense.at[i], sem.at[i])

    def put(i):
        at = slice(i * group, (i + 1) * group)
        return pltpu.make_async_copy(spread.at[at, :], spread_hbm.at[at, :], out_sem.at[i])

    for i in range(2 * pairs):
        fetch(i).start()
    high = mix[...].astype(BF16)
    low = (mix[...] - high.astype(F32)).astype(BF16)
    owner = lax.broadcasted_iota(jnp.int32, (block, deep), 1) // fields
    mine = owner == lax.broadcasted_iota(jnp.int32, (block, deep), 0)
    picks = jnp.concatenate(
        [jnp.where(mine, high.astype(F32), 0.0), jnp.where(mine, low.astype(F32), 0.0)], 0
    ).astype(BF16)

    def step(i, carry):
        fetch(2 * i).wait()
        fetch(2 * i + 1).wait()
        even = dot(picks, dense[2 * i])
        odd = dot(picks, dense[2 * i + 1])
        both = jnp.concatenate([even[:block] + even[block:], odd[:block] + odd[block:]], 0)
        at = span(i, 2 * block)
        mixed_t[:, at] = both.T
        mixed[at, :] = both.astype(BF16)
        return carry

    for g in range(2):
        lax.fori_loop(g * pairs // 2, (g + 1) * pairs // 2, step, 0)
        at = slice(g * group, (g + 1) * group)
        spread[at, :] = lax.dot_general(
            mixed[at, :], w_out[...], (((1,), (1,)), ((), ())), preferred_element_type=F32
        ).astype(BF16)
        put(g).start()
    for g in range(2):
        put(g).wait()


def logit_body(total_rows, arrived, gain, bias, base, hidden_hbm, spread_hbm, coef, parts, hidden, spread, sem):
    rows, units = hidden.shape
    block = LANES
    blocks = rows // block

    for i in range(blocks):
        rows_in(hidden_hbm, hidden, sem, 0, i, block).start()
        rows_in(spread_hbm, spread, sem, 1, i, block).start()
    stats = jnp.sum(arrived[...], 0)
    mean = stats[0:1] / total_rows
    var = stats[1:2] / total_rows - mean * mean
    inv = lax.rsqrt(var + epsilon)
    coef[0:1, :] = gain[...] * inv
    coef[1:2, :] = bias[...]
    coef[2:3, :] = mean - base[...]
    coef[3:4, :] = inv

    def step(i, carry):
        at = span(i, block)
        rows_in(hidden_hbm, hidden, sem, 0, i, block).wait()
        rows_in(spread_hbm, spread, sem, 1, i, block).wait()
        total = jnp.zeros((block, LANES), F32)
        for n in range(units // LANES):
            cols = slice(n * LANES, (n + 1) * LANES)
            value = (hidden[at, cols].astype(F32) - coef[2:3, cols]) * coef[0:1, cols] + coef[1:2, cols]
            total = total + value * spread[at, cols].astype(F32)
        line = jnp.sum(total.T, 0, keepdims=True)
        for k in range(parts.shape[0]):
            parts[k, pl.ds(i, 1), :] = line
        return carry

    lax.fori_loop(0, blocks, step, 0)


def column(line):
    return jnp.broadcast_to(line, (LANES, LANES)).T


def two_parts(value):
    high = value.astype(BF16)
    return high, (value - high.astype(F32)).astype(BF16)


def grad_body(total_rows, arrived, labels, hidden_hbm, spread_hbm, coef, mixed_t, grads, packed, hidden, spread,
              normed, weighted, totals, sem):
    rows, units = hidden.shape
    emb = mixed_t.shape[0]
    block = LANES
    blocks = rows // block
    own = packed.shape[0]
    share = units // own
    for i in range(blocks):
        rows_in(hidden_hbm, hidden, sem, 0, i, block).start()
        rows_in(spread_hbm, spread, sem, 1, i, block).start()
    logits = jnp.sum(arrived[...], 0)
    targets = labels[...]
    positive = jnp.maximum(logits, 0.0) + jnp.log1p(jnp.exp(-jnp.abs(logits)))
    loss = jnp.sum(positive - targets * logits, keepdims=True)
    grads[...] = (jax.nn.sigmoid(logits) - targets) * (grad_scale / math.sqrt(total_rows))
    for i in range(blocks):
        at = slice(i * block, (i + 1) * block)
        weighted[:, at] = (mixed_t[:, at] * grads[i : i + 1, :]).astype(BF16)
    totals[...] = jnp.zeros_like(totals)

    def step(i, carry):
        at = span(i, block)
        rows_in(hidden_hbm, hidden, sem, 0, i, block).wait()
        rows_in(spread_hbm, spread, sem, 1, i, block).wait()
        weight = column(grads[pl.ds(i, 1), :])
        for n in range(units // LANES):
            cols = slice(n * LANES, (n + 1) * LANES)
            part = weight * spread[at, cols].astype(F32)
            centred = hidden[at, cols].astype(F32) - coef[2:3, cols]
            normed[at, cols] = (centred * coef[0:1, cols] + coef[1:2, cols]).astype(BF16)
            product = part * centred
            totals[0:8, cols] += part.reshape(block // 8, 8, LANES).sum(0)
            totals[8:16, cols] += product.reshape(block // 8, 8, LANES).sum(0)
        return carry

    lax.fori_loop(0, blocks, step, 0)
    bias = jnp.sum(totals[0:8, :], 0, keepdims=True)
    gain = jnp.sum(totals[8:16, :], 0, keepdims=True) * coef[3:4, :]
    cuts = [slice(q * emb, (q + 1) * emb) for q in range(units // emb)]
    lines = jnp.concatenate([bias[:, c] for c in cuts] + [gain[:, c] for c in cuts], 0)
    spare = [v.astype(F32) for v in two_parts(jnp.broadcast_to(loss, (1, emb)))]
    extra = jnp.concatenate(spare + [jnp.zeros((6, emb), F32)], 0).astype(BF16)
    for p, block_of in enumerate((*two_parts(lines), extra)):
        for k in range(own):
            packed[k, share + 8 * p : share + 8 * p + 8, :] = block_of
    for n in range(units // 512):
        cols = slice(n * 512, (n + 1) * 512)
        out = dot(weighted[...], normed[:, cols]).T.astype(BF16)
        for k in range(512 // share):
            packed[n * (512 // share) + k, 0:share, :] = out[k * share : (k + 1) * share, :]


def lefts(turned_hbm, left, sem, z_chunk, x_chunk):
    quarter = left.shape[1]
    sub = quarter // 4
    copies = [pltpu.make_async_copy(turned_hbm.at[span(z_chunk, quarter), :], left.at[0], sem.at[0])]
    for q in range(4):
        at = pl.ds(pl.multiple_of(q * quarter + x_chunk * sub, sub), sub)
        copies.append(pltpu.make_async_copy(turned_hbm.at[at, :], left.at[1, q * sub : (q + 1) * sub, :], sem.at[1 + q]))
    return copies


def ahead_body(chunks, grads, hidden_hbm, spread_hbm, slope_hbm, coef, turned_hbm, terms_hbm, hidden, spread, slope, plain,
               flat, tilted, left, terms, sem, left_sem, out_sem):
    rows, units = hidden.shape
    block = LANES
    blocks = rows // block
    wide = units // 2
    far = lefts(turned_hbm, left, left_sem, chunks[2], chunks[6])
    for i in range(blocks):
        rows_in(hidden_hbm, hidden, sem, 0, i, block).start()
        rows_in(spread_hbm, spread, sem, 1, i, block).start()
        rows_in(slope_hbm, slope, sem, 2, i, block).start()
    for copy in far:
        copy.start()

    def step(i, carry):
        at = span(i, block)
        rows_in(hidden_hbm, hidden, sem, 0, i, block).wait()
        rows_in(spread_hbm, spread, sem, 1, i, block).wait()
        rows_in(slope_hbm, slope, sem, 2, i, block).wait()
        weight = column(grads[pl.ds(i, 1), :])
        for n in range(units // LANES):
            cols = slice(n * LANES, (n + 1) * LANES)
            factor = coef[0:1, cols] * slope[at, cols].astype(F32)
            flat[at, cols] = factor.astype(BF16)
            plain[at, cols] = (factor * (weight * spread[at, cols].astype(F32))).astype(BF16)
            tilted[at, cols] = (factor * (hidden[at, cols].astype(F32) - coef[2:3, cols])).astype(BF16)
        return carry

    lax.fori_loop(0, blocks, step, 0)
    for copy in far:
        copy.wait()

    def put(k):
        return pltpu.make_async_copy(terms.at[k], terms_hbm.at[k], out_sem.at[k])

    for axis in range(2):
        cols = slice(axis * wide, (axis + 1) * wide)
        for k, right in enumerate((plain, flat, tilted)):
            terms[3 * axis + k] = dot(left[axis], right[:, cols]).astype(BF16)
            put(3 * axis + k).start()
    for k in range(6):
        put(k).wait()


def lay_piece(message, piece, below):
    half = piece.shape[0] // 2
    wide = piece.shape[1]
    for n in range(2):
        message[below:, n * wide : (n + 1) * wide] = piece[n * half : (n + 1) * half, :]


def far_body(total_rows, arrived, coef, terms_hbm, z_hbm, x_hbm, both, piece, terms, held_z, held_x, sem, out_sem):
    units = coef.shape[1]
    share, emb = piece.shape
    quarter, wide = terms.shape[1:]
    held = (held_z, held_x)

    def get(k):
        return pltpu.make_async_copy(terms_hbm.at[k], terms.at[k], sem.at[k])

    def put(axis):
        return pltpu.make_async_copy(held[axis], (z_hbm, x_hbm)[axis], out_sem.at[axis])

    for k in range(6):
        get(k).start()
    count = units // emb

    def stat(p):
        return jnp.sum(arrived[:, share + 8 * p : share + 8 * p + 8, :].astype(F32), 0)

    lines = stat(1) + stat(0)
    for q in range(count):
        cols = slice(q * emb, (q + 1) * emb)
        both[2:3, cols] = lines[q : q + 1]
        both[3:4, cols] = lines[count + q : count + q + 1]
        both[0:1, cols] = lines[q : q + 1] / total_rows
        both[1:2, cols] = lines[count + q : count + q + 1] * coef[3:4, cols] / total_rows
    both[4:5, 0:emb] = jnp.sum(stat(2), 0, keepdims=True) / total_rows
    piece[...] = jnp.sum(arrived[:, 0:share, :].astype(F32), 0).astype(BF16)
    for axis in range(2):
        if axis == 1:
            lay_piece(held_x, piece, quarter)
        for k in range(3):
            get(3 * axis + k).wait()
        for r in range(quarter // LANES):
            at = slice(r * LANES, (r + 1) * LANES)
            for n in range(wide // LANES):
                cols = slice(n * LANES, (n + 1) * LANES)
                here = slice(axis * wide + n * LANES, axis * wide + (n + 1) * LANES)
                value = terms[3 * axis, at, cols].astype(F32) - terms[3 * axis + 1, at, cols].astype(F32) * both[0:1, here]
                value = value - terms[3 * axis + 2, at, cols].astype(F32) * both[1:2, here]
                held[axis][at, cols] = value.astype(BF16)
        put(axis).start()
    for axis in range(2):
        put(axis).wait()


def product(axis, chunk, turned, grad_pre, piece, lines, out):
    rows, wide = lines.shape[0], out.shape[1]
    sub = rows // 4
    if axis == 0:
        left = turned[span(chunk, rows), :]
    else:
        for q in range(4):
            at = pl.ds(pl.multiple_of(q * rows + chunk * sub, sub), sub)
            lines[q * sub : (q + 1) * sub, :] = turned[at, :]
        left = lines[...]
        lay_piece(out, piece, rows)
    out[0:rows, :] = dot(left, grad_pre[:, axis * wide : (axis + 1) * wide]).astype(BF16)


def back_body(grads, hidden_hbm, spread_hbm, slope_hbm, coef, both, grad_pre, grad_gain, grad_bias, loss, hidden, spread, slope,
              sem):
    rows, units = hidden.shape
    block = LANES
    blocks = rows // block
    for i in range(blocks):
        rows_in(hidden_hbm, hidden, sem, 0, i, block).start()
        rows_in(spread_hbm, spread, sem, 1, i, block).start()
        rows_in(slope_hbm, slope, sem, 2, i, block).start()
    grad_bias[...] = both[2:3, :]
    grad_gain[...] = both[3:4, :]
    loss[...] = both[4:5, 0:LANES]

    def step(i, carry):
        at = span(i, block)
        rows_in(hidden_hbm, hidden, sem, 0, i, block).wait()
        rows_in(spread_hbm, spread, sem, 1, i, block).wait()
        rows_in(slope_hbm, slope, sem, 2, i, block).wait()
        weight = column(grads[pl.ds(i, 1), :])
        for n in range(units // LANES):
            cols = slice(n * LANES, (n + 1) * LANES)
            inner = weight * spread[at, cols].astype(F32) - both[0:1, cols]
            inner = inner - (hidden[at, cols].astype(F32) - coef[2:3, cols]) * both[1:2, cols]
            grad_pre[at, cols] = (inner * coef[0:1, cols] * slope[at, cols].astype(F32)).astype(BF16)
        return carry

    lax.fori_loop(0, blocks, step, 0)


def near_body(step_on, chunks, turned, grad_pre, piece, after, z_hbm, x_hbm, lines, z, x, out_sem):
    del after
    jobs = ((z, z_hbm), (x, x_hbm))

    def put(axis):
        return pltpu.make_async_copy(*jobs[axis], out_sem.at[axis])

    for axis in range(2):
        product(axis, chunks[4 * axis + step_on], turned, grad_pre, piece, lines, jobs[axis][0])
        put(axis).start()
    for axis in range(2):
        put(axis).wait()


def own_body(chunks, turned, grad_pre, piece, after, z0, x0, lines):
    del after
    product(0, chunks[0], turned, grad_pre, piece, lines, z0)
    product(1, chunks[4], turned, grad_pre, piece, lines, x0)


def middle_body(chunk, own, far, up, down, own_out, far_out, up_out, down_out):
    me, was = chunk[0], chunk[1]
    rows = own_out.shape[0]
    full = own.shape[0] - (far_out.shape[0] - rows) // 4
    some = (far_out.shape[0] - rows) // 4
    for step, out in ((2, far_out), (1, up_out), (3, down_out), (0, own_out)):
        at = span(lax.rem(me + step, 4), rows)
        total = (own[at, :].astype(F32) + far[at, :].astype(F32)) + (up[at, :].astype(F32) + down[at, :].astype(F32))
        out[0:rows, :] = total.astype(out.dtype)
        if step and some:
            for back, came in ((0, own), (2, far), (1, up), (3, down)):
                to = pl.ds(pl.multiple_of(rows + lax.rem(was + 4 - back, 4) * some, some), some)
                out[to, :] = came[full:, :]


def last_body(place, own_a, a2, a1, a3, own_b, b0, b2, b1, b3, hash_hbm, out_hbm, grad_hash, grad_out, sem):
    rows, half = own_a.shape
    some = (b0.shape[0] - rows) // 4
    share = 2 * some
    emb = grad_out.shape[1]
    for back, came in zip((0, 2, 1, 3), (b0, b2, b1, b3)):
        there = lax.rem(place[0] + 4 - back, 4)
        for k in range(4):
            for n in range(2):
                to = pl.ds(pl.multiple_of((there * 4 + k) * share + n * some, some), some)
                at = slice(rows + k * some, rows + (k + 1) * some)
                grad_out[to, :] = came[at, n * emb : (n + 1) * emb].astype(F32)
    put_out = pltpu.make_async_copy(grad_out, out_hbm, sem.at[0])
    put_out.start()
    for base, own, came in ((0, own_a, (a2, a1, a3)), (half, own_b, (b2, b1, b3))):
        total = own[...]
        for part in came:
            total = total + part[0:rows, :].astype(F32)
        grad_hash[:, base : base + half] = total
    put_hash = pltpu.make_async_copy(grad_hash, hash_hbm, sem.at[1])
    put_hash.start()
    put_out.wait()
    put_hash.wait()


def on_device(hash_codes, w_hash, norm_gain, norm_bias, w_out, dense_vectors, field_mix, labels):
    rows, codes = hash_codes.shape
    units = w_hash.shape[1]
    fields, emb = dense_vectors.shape[1:]
    dp, mp = lax.axis_size(DP), lax.axis_size(MP)
    total_rows = rows * dp
    lines = rows // LANES
    half = units // 2
    share = units // dp
    some = share // 4
    dma = pltpu.SemaphoreType.DMA
    hidden, slope, sums, base = call(
        decode_body,
        [(hash_codes, "h"), (w_hash, "h")],
        [((rows, units), BF16, "h"), ((rows, units), BF16, "h"), ((dp, 2, units), F32, "h"), ((1, units), F32, "v")],
        [
            pltpu.VMEM((rows, codes), jnp.int32),
            pltpu.VMEM((codes, units), BF16),
            pltpu.VMEM((rows, units), BF16),
            pltpu.VMEM((rows, units), BF16),
            pltpu.VMEM((rows, codes), BF16),
            pltpu.VMEM((256, units // 2), F32),
            pltpu.VMEM((256, units // 2), F32),
            pltpu.VMEM((256, units), F32),
            pltpu.VMEM((16, units), F32),
            pltpu.VMEM((dp, 2, units), F32),
            dma((rows // 256,)),
            dma((2,)),
            dma((2, rows // 256)),
            dma((1,)),
        ],
        flops=2 * rows * codes * units,
        limit=40,
    )
    arrived = exchange(sums, DP)
    mix_line = jnp.tile(field_mix / math.sqrt(emb), 64).reshape(1, fields * 64)
    spread, mixed_t = call(
        mix_body,
        [(sums, "h"), (dense_vectors.reshape(rows * fields, emb), "h"), (mix_line, "v"), (w_out, "v")],
        [((rows, units), BF16, "h"), ((emb, rows), F32, "v")],
        [
            pltpu.VMEM((rows // 64, fields * 64, emb), BF16),
            pltpu.VMEM((rows, emb), BF16),
            pltpu.VMEM((rows, units), BF16),
            dma((rows // 64,)),
            dma((2,)),
        ],
        flops=8 * rows * units * emb,
        limit=16,
    )
    coef, parts = call(
        functools.partial(logit_body, float(total_rows)),
        [
            (arrived, "v"),
            (norm_gain.reshape(1, units), "v"),
            (norm_bias.reshape(1, units), "v"),
            (base, "v"),
            (hidden, "h"),
            (spread, "h"),
        ],
        [((8, units), F32, "v"), ((mp, lines, LANES), F32, "v")],
        [pltpu.VMEM((rows, units), BF16), pltpu.VMEM((rows, units), BF16), dma((2, lines))],
        limit=20,
        flops=4 * rows * units,
    )
    logits = exchange(parts, MP)
    (turned,) = call(
        turn_body,
        [(hash_codes, "h"), (parts, "h")],
        [((codes, rows), BF16, "h")],
        [pltpu.VMEM((rows, codes), jnp.int32), pltpu.VMEM((codes, rows), BF16), dma((1, lines)), dma((lines,))],
        flops=16 * rows * codes * LANES,
        limit=16,
    )
    targets = labels.astype(F32).reshape(lines, LANES)
    grads, packed = call(
        functools.partial(grad_body, float(total_rows)),
        [(logits, "v"), (targets, "v"), (hidden, "h"), (spread, "h"), (coef, "v"), (mixed_t, "v")],
        [((lines, LANES), F32, "v"), ((dp, share + 24, emb), BF16, "v")],
        [
            pltpu.VMEM((rows, units), BF16),
            pltpu.VMEM((rows, units), BF16),
            pltpu.VMEM((rows, units), BF16),
            pltpu.VMEM((emb, rows), BF16),
            pltpu.VMEM((16, units), F32),
            dma((2, lines)),
        ],
        limit=24,
        flops=2 * rows * units * emb,
    )
    grad_arrived = exchange(packed, DP)
    here = {axis: lax.axis_index(axis).astype(jnp.int32) for axis in DP}
    chunks = jnp.stack([(here[axis] + step) & 3 for axis in DP for step in range(4)])
    sizes = ((codes // 4, half), (codes // 4 + 2 * some, half))
    (terms,) = call(
        ahead_body,
        [
            (chunks, "s"),
            (grads, "v"),
            (hidden, "h"),
            (spread, "h"),
            (slope, "h"),
            (coef, "v"),
            (turned, "h"),
        ],
        [((6, codes // 4, half), BF16, "h")],
        [pltpu.VMEM((rows, units), BF16)] * 6
        + [
            pltpu.VMEM((2, codes // 4, rows), BF16),
            pltpu.VMEM((6, codes // 4, half), BF16),
            dma((3, lines)),
            dma((5,)),
            dma((6,)),
        ],
        flops=6 * rows * half * codes,
        limit=30,
    )
    far_z, far_x, both, piece = call(
        functools.partial(far_body, float(total_rows)),
        [(grad_arrived, "v"), (coef, "v"), (terms, "h")],
        [
            (sizes[0], BF16, "h"),
            (sizes[1], BF16, "h"),
            ((8, units), F32, "p"),
            ((share, emb), BF16, "p"),
        ],
        [pltpu.VMEM((6, codes // 4, half), BF16)] + [pltpu.VMEM(size, BF16) for size in sizes] + [dma((6,)), dma((2,))],
        limit=10,
        flops=8 * rows * units,
    )
    grad_pre, grad_gain, grad_bias, loss = call(
        back_body,
        [(grads, "v"), (hidden, "h"), (spread, "h"), (slope, "h"), (coef, "v"), (both, "p")],
        [((rows, units), BF16, "p"), ((1, units), F32, "v"), ((1, units), F32, "v"), ((1, LANES), F32, "v")],
        [pltpu.VMEM((rows, units), BF16)] * 3 + [dma((3, lines))],
        limit=20,
        flops=8 * rows * units,
    )

    def near(step_on, after):
        return call(
            functools.partial(near_body, step_on),
            [(chunks, "s"), (turned, "p"), (grad_pre, "p"), (piece, "p"), (after, "h")],
            [(size, BF16, "h") for size in sizes],
            [pltpu.VMEM((codes // 4, rows), BF16)] + [pltpu.VMEM(size, BF16) for size in sizes] + [dma((2,))],
            flops=rows * half * codes,
            limit=8,
        )

    up = near(1, terms)
    down = near(3, up[0])
    own_z, own_x = call(
        own_body,
        [(chunks, "s"), (turned, "p"), (grad_pre, "p"), (piece, "p"), (down[0], "h")],
        [(size, BF16, "p") for size in sizes],
        [pltpu.VMEM((codes // 4, rows), BF16)],
        limit=4,
        flops=rows * half * codes,
    )
    made = {("z", 2): far_z, ("x", 2): far_x, ("z", 0): own_z, ("x", 0): own_x}
    made.update(zip((("z", 1), ("x", 1), ("z", 3), ("x", 3)), (*up, *down)))
    got = {(axis, step): hop(made[axis, step], axis, step) for step in (2, 1, 3) for axis in DP}
    other = {"z": "x", "x": "z"}
    last = []
    for axis in DP:
        own, far, up, down = call(
            middle_body,
            [(jnp.stack([here[other[axis]], here[axis]]), "s"), (made[axis, 0], "p")]
            + [(got[axis, step], "p") for step in (2, 1, 3)],
            [((codes // 16, half), F32, "p")] + [((codes // 16 + 8 * some * (axis == "x"), half), BF16, "p")] * 3,
            limit=4,
            flops=rows * units,
        )
        last += [own] + [far] * (axis == "x") + [hop(v, other[axis], step) for v, step in ((far, 2), (up, 1), (down, 3))]
    grad_hash, grad_out = call(
        last_body,
        [(jnp.stack([here["z"], here["x"]]), "s")] + [(v, "p") for v in last],
        [((codes // 16, units), F32, "h"), ((units, emb), F32, "h")],
        [pltpu.VMEM((codes // 16, units), F32), pltpu.VMEM((units, emb), F32), dma((2,))],
        limit=8,
        flops=rows * units,
    )
    return (grad_hash, grad_gain.reshape(units), grad_bias.reshape(units), grad_out, loss[0, 0])


def solution(mesh):
    split = Mesh(mesh.devices.reshape(4, 4, 4, 2), ("z", "x", "y", "core"))
    return jax.shard_map(
        on_device,
        mesh=split,
        in_specs=(P(DP, None), P(None, MP), P(MP), P(MP), P(MP, None), P(DP, None, None), P(), P(DP)),
        out_specs=(P(DP, MP), P(MP), P(MP), P(MP, None), P()),
        check_vma=False,
    )
```
